512 devices in a mesh: text: 16 (over z, y_lo), det: 32 (over y_hi, x, core).
Axes of the slice: x: 4, y: 8 (y_hi: 4, y_lo: 2; y = y_hi * 2 + y_lo), z: 8, core: 2. Of those that a mesh axis runs over, the one named last changes fastest.
Arguments:
- prompt_embeds: bfloat16 [256, 16, 2048], P('text'), may hold values from -6 to 6
- prompt_len: int32 [256], P('text'), may hold values from 1 to 16
- norm_gain: float32 [2048], replicated, may hold values from 0.5 to 1.5
- w_up: bfloat16 [2048, 8192], P(None, 'det'), may hold values from -0.125 to 0.125
- w_down: bfloat16 [8192, 2048], P('det'), may hold values from -0.0625 to 0.0625
- final_gain: float32 [2048], replicated, may hold values from 0.25 to 1.75
- w_proj: bfloat16 [2048, 256], P('det'), may hold values from -0.125 to 0.125
- queries: bfloat16 [512, 1100, 256], P(('text', 'det')), may hold values from -6 to 6
- assign: int32 [512, 1100], P(('text', 'det')), may hold values from 0 to 511
- valid: int32 [512, 256], P(('text', 'det')), may hold values 0 or 1
Outputs:
- grad_up: float32 [2048, 8192], P('text', 'det')
- grad_down: float32 [8192, 2048], P('det', 'text')
- grad_proj: float32 [2048, 256], P('det')
- grad_queries: float32 [512, 1100, 256], P(('text', 'det'))
The draws below stay inside these ranges and needn't reach their ends.
Inputs may be any that keep to these rules, and one draw needn't show every extreme that they name: `prompt_len`: every prompt uses at least its first token. `assign`: A value of 256 or more means the query has no concept.
All inputs are finite; a program needn't handle non-finite values. No bound on the sum of `valid` on one device may be relied on, other than what follows from the above.
Results may differ from the reference program's by a relative error of at most 0.025.
Values may be sent and summed in bfloat16 or wider, within the bound.
A program may use at most 64 MiB of HBM per device.

```python
import jax
import jax.numpy as jnp
from jax import lax

D = 2048
HID = 8192
DQ = 256
PROMPT = 16
QUERIES = 1100
CON_DEV = 16
CONCEPTS = 256
IMAGES = 512
N_TEXT = 16


def place_ends(array, own_key, low, largest):
    longest = array.shape.index(max(array.shape))
    spots = []
    for shift in (0, 1):
        where = [jax.random.randint(jax.random.fold_in(own_key, axis), (), 0, length) for axis, length in enumerate(array.shape)]
        where[longest] = (where[longest] + shift) % array.shape[longest]
        spots.append(tuple(where))
    return array.at[spots[0]].set(low).at[spots[1]].set(largest)


def block_levels(rng, dims, shards, low, largest):
    def one(dim, blocks):
        draws = jax.random.uniform(jax.random.fold_in(jax.random.fold_in(rng, 6), dim), (blocks,), jnp.float32, low / len(shards), largest / len(shards))
        return jnp.repeat(jnp.exp(draws), dims[dim] // blocks).reshape((-1,) + (1,) * (len(dims) - dim - 1))

    gain = one(*shards[0])
    for cut in shards[1:]:
        gain = gain * one(*cut)
    return gain


def normal_values(key, extent, width, limit, shards=(), dtype=jnp.bfloat16):
    entries = jax.random.normal(key, extent, jnp.float32) * width
    if len(shards) > 0:
        entries = block_levels(key, extent, shards, -0.22, 0.18) * entries
    return jnp.clip(entries, min=-limit, max=limit).astype(dtype)


def setup_inputs(seed: int = 0) -> dict:
    splits = jax.random.split(jax.random.key(seed), 11)
    prompt_embeds = normal_values(splits[0], (CONCEPTS, PROMPT, D), 1.0, 6.0, ((0, 16),))
    prompt_len = place_ends(jax.random.randint(splits[1], (CONCEPTS,), 1, PROMPT + 1), jax.random.fold_in(splits[1], 1), 1, PROMPT).astype(jnp.int32)
    norm_gain = jnp.clip(1.0 + 0.1 * jax.random.normal(splits[2], (D,), jnp.float32), 0.5, 1.5)
    w_up = normal_values(splits[3], (D, HID), D ** -0.5, 0.125, ((1, 32),))
    w_down = normal_values(splits[4], (HID, D), HID ** -0.5, 0.0625, ((0, 32),))
    final_gain = jnp.clip(1.0 + 0.15 * jax.random.normal(splits[5], (D,), jnp.float32), 0.25, 1.75)
    w_proj = normal_values(splits[6], (D, DQ), D ** -0.5, 0.125, ((0, 32),))
    queries = normal_values(splits[7], (IMAGES, QUERIES, DQ), 1.0, 6.0, ((0, 512),))
    assign = place_ends(jax.random.randint(splits[8], (IMAGES, QUERIES), 0, 2 * CONCEPTS), jax.random.fold_in(splits[8], 1), 0, (2 * CONCEPTS) - 1).astype(jnp.int32)
    valid = place_ends((jax.random.randint(splits[9], (IMAGES, CONCEPTS), 0, 16) < 1).astype(jnp.int32), jax.random.fold_in(splits[9], 1), 0, 1)
    return dict(prompt_embeds=prompt_embeds, prompt_len=prompt_len, norm_gain=norm_gain, w_up=w_up, w_down=w_down, final_gain=final_gain, w_proj=w_proj, queries=queries, assign=assign, valid=valid)


EPS = 1e-05
ALPHA = 0.25
LOGIT_BIAS = -2.0

def gelu_fn(values):
    return jax.nn.gelu(values, approximate=True)

def focal_total(scores, target, weight):
    log_pos = jax.nn.log_sigmoid(scores)
    log_neg = jax.nn.log_sigmoid(-scores)
    probab = jax.nn.sigmoid(scores)
    pos_term = -ALPHA * target * (1.0 - probab) ** 2 * log_pos
    neg_term = -(1.0 - ALPHA) * (1.0 - target) * probab ** 2 * log_neg
    return jnp.sum(weight * (pos_term + neg_term))

def norm_parts(values):
    row_mean = lax.optimization_barrier(jnp.mean(values, axis=-1, keepdims=True))
    centred = values - row_mean
    variance = lax.optimization_barrier(jnp.mean(centred * centred, axis=-1, keepdims=True))
    inv_scale = lax.rsqrt(variance + EPS)
    return (centred * inv_scale, inv_scale)

def reference(prompt_embeds, prompt_len, norm_gain, w_up, w_down, final_gain, w_proj, queries, assign, valid):
    tok_rows = CONCEPTS * PROMPT
    tokens = prompt_embeds.reshape(tok_rows, D).astype(jnp.float32)
    in_hat, _ = norm_parts(tokens)
    normed = (in_hat * norm_gain).astype(jnp.bfloat16)
    pre_act = jnp.dot(normed, w_up, preferred_element_type=jnp.float32)
    hidden_act, act_back = jax.vjp(gelu_fn, pre_act)
    hidden = hidden_act.astype(jnp.bfloat16)
    layer_out = tokens + jnp.dot(hidden, w_down, preferred_element_type=jnp.float32)
    out_hat, inv_scale = norm_parts(layer_out)
    final = out_hat * final_gain
    position = lax.broadcasted_iota(jnp.int32, (CONCEPTS, PROMPT), 1)
    lengths = prompt_len.astype(jnp.float32)
    pool_weight = (position < prompt_len[:, None]).astype(jnp.float32) / lengths[:, None]
    pooled = lax.optimization_barrier(jnp.sum(final.reshape(CONCEPTS, PROMPT, D) * pool_weight[:, :, None], axis=1))
    pooled_low = pooled.astype(jnp.bfloat16)
    concept_feat = jnp.dot(pooled_low, w_proj, preferred_element_type=jnp.float32).astype(jnp.bfloat16)
    score_scale = DQ ** (-0.5)

    def per_image(summed, item_parts):
        query_rows, chosen, allowed = item_parts
        scores = jnp.dot(query_rows, concept_feat.T, preferred_element_type=jnp.float32) * score_scale + LOGIT_BIAS
        column = lax.broadcasted_iota(jnp.int32, (QUERIES, CONCEPTS), 1)
        target = (chosen[:, None] == column).astype(jnp.float32)
        weight = jnp.broadcast_to(allowed[None, :].astype(jnp.float32), (QUERIES, CONCEPTS))
        score_grad = jax.grad(focal_total)(scores, target, weight).astype(jnp.bfloat16)
        query_grad = jnp.dot(score_grad, concept_feat, preferred_element_type=jnp.float32) * score_scale
        terms = jnp.dot(score_grad.T, query_rows, preferred_element_type=jnp.float32)
        return (summed + terms, query_grad)
    summed, grad_queries = lax.scan(per_image, jnp.zeros((CONCEPTS, DQ), jnp.float32), (queries, assign, valid))
    feat_grad = summed * (score_scale / IMAGES)
    grad_proj = jnp.dot(pooled_low.astype(jnp.float32).T, feat_grad, precision=lax.Precision.HIGHEST)
    pooled_grad = jnp.dot(feat_grad, w_proj.astype(jnp.float32).T, precision=lax.Precision.HIGHEST)
    final_grad = (pooled_grad[:, None, :] * pool_weight[:, :, None]).reshape(tok_rows, D)
    hat_grad = final_grad * final_gain
    mean_first = lax.optimization_barrier(jnp.mean(hat_grad, axis=-1, keepdims=True))
    mean_second = lax.optimization_barrier(jnp.mean(hat_grad * out_hat, axis=-1, keepdims=True))
    out_grad = ((hat_grad - mean_first - out_hat * mean_second) * inv_scale).astype(jnp.bfloat16)
    hidden_grad = jnp.dot(out_grad, w_down.T, preferred_element_type=jnp.float32)
    pre_grad = act_back(hidden_grad)[0].astype(jnp.bfloat16)
    group_rows = CON_DEV * PROMPT

    def group_sum(carry, item_parts):
        down_sum, up_sum = carry
        hidden_part, out_part, normed_part, pre_part = item_parts
        down_part = jnp.dot(hidden_part.T, out_part, preferred_element_type=jnp.float32)
        up_part = jnp.dot(normed_part.T, pre_part, preferred_element_type=jnp.float32)
        down_round = lax.optimization_barrier(down_part.astype(jnp.bfloat16)).astype(jnp.float32)
        up_round = lax.optimization_barrier(up_part.astype(jnp.bfloat16)).astype(jnp.float32)
        return ((down_sum + down_round, up_sum + up_round), None)
    start = (jnp.zeros((HID, D), jnp.float32), jnp.zeros((D, HID), jnp.float32))
    pieces = (hidden.reshape(N_TEXT, group_rows, HID), out_grad.reshape(N_TEXT, group_rows, D), normed.reshape(N_TEXT, group_rows, D), pre_grad.reshape(N_TEXT, group_rows, HID))
    (grad_down, grad_up), _ = lax.scan(group_sum, start, pieces)
    return (grad_up, grad_down, grad_proj, grad_queries)
```

```python
import jax
import jax.numpy as jnp
from jax import lax
from jax.experimental import pallas as pl
from jax.experimental.pallas import tpu as pltpu
from jax.sharding import PartitionSpec as P

EPS = 1e-05
ALPHA = 0.25
LOGIT_BIAS = -2.0
F32 = jnp.float32
BF16 = jnp.bfloat16
MESH = pl.DeviceIdType.MESH
GC = 0.7978845608028654
GA = 0.044715


class Place:
    def __init__(self):
        self.t = lax.axis_index("text")
        self.d = lax.axis_index("det")
        self.core = lax.rem(self.d, 2)
        self.chip = self.d // 2
        self.x = lax.rem(self.chip, 4)
        self.y = self.chip // 4
        self.z = self.t // 2
        self.yl = lax.rem(self.t, 2)

    def other_core(self):
        return {"det": self.d + 1 - 2 * self.core}

    def along_x(self, i):
        return {"det": (self.y * 4 + lax.rem(self.x + i, 4)) * 2 + self.core}

    def along_y(self, i):
        return {"det": (lax.rem(self.y + i, 4) * 4 + self.x) * 2 + self.core}

    def in_plane(self, i):
        return {"det": lax.rem(self.chip + i, 16) * 2 + self.core}

    def in_text(self, i):
        return {"text": lax.rem(self.t + i, 16)}

    def along_z(self, i):
        return {"text": lax.rem(self.z + i, 8) * 2 + self.yl}

    def across(self):
        return {"text": self.t + 1 - 2 * self.yl}

    def greet(self):
        barrier = pltpu.get_barrier_semaphore()
        pl.semaphore_signal(barrier, inc=1, device_id=self.other_core(), device_id_type=MESH)
        for i in range(1, 16):
            pl.semaphore_signal(barrier, inc=1, device_id=self.in_plane(i), device_id_type=MESH)
            pl.semaphore_signal(barrier, inc=1, device_id=self.in_text(i), device_id_type=MESH)

    def met(self):
        pl.semaphore_wait(pltpu.get_barrier_semaphore(), 31)


class Sends:
    def __init__(self, send_sems, recv_sems):
        self.send_sems, self.recv_sems, self.used = send_sems, recv_sems, 0
        self.flying = []

    def __call__(self, src, dst, to):
        copy = pltpu.make_async_remote_copy(
            src_ref=src,
            dst_ref=dst,
            send_sem=self.send_sems.at[self.used],
            recv_sem=self.recv_sems.at[self.used],
            device_id=to,
            device_id_type=MESH,
        )
        self.used += 1
        copy.start()
        self.flying.append(copy)
        return copy

    def drain(self):
        for copy in self.flying:
            copy.wait_send()


def at(i, n):
    return pl.ds(pl.multiple_of(i * n, n), n)


def dot(a, b, dims=((1,), (0,))):
    return lax.dot_general(a, b, (dims, ((), ())), preferred_element_type=F32)


def pool_weights(plen_ref, chip):
    length = jnp.full((16, 128), plen_ref[chip], jnp.int32)
    slot = lax.broadcasted_iota(jnp.int32, (16, 128), 0)
    weight = jnp.where(slot < length, 1.0 / length.astype(F32), 0.0)
    return weight[:, :1]


A_COPIES = 2 + 6 + 6 + 1 + 3 + 3 + 1 + 15 + 15 + 15


def forward_kernel(
    plen, tok, ngain, w_up, w_down, fgain, w_proj,
    feat_o, hid_o, nrm_o, gd_o, oh_o, inv_o, pool_o, wfull_o,
    cs, cr, xs, xr, ys, yr, lo, wfull, frow, psend, prow, allf, send_sems, recv_sems,
):
    me = Place()
    send = Sends(send_sems, recv_sems)
    core, chip, x, y, t = me.core, me.chip, me.x, me.y, me.t
    me.greet()
    tokens = tok[...].astype(F32)
    centred = tokens - jnp.mean(tokens, axis=1, keepdims=True)
    variance = jnp.mean(centred * centred, axis=1, keepdims=True)
    normed = (centred * lax.rsqrt(variance + EPS) * ngain[...]).astype(BF16)
    nrm_o[...] = normed
    pre = dot(normed, w_up[...])
    tanh = jnp.tanh(GC * (pre + GA * pre * pre * pre))
    hidden = (0.5 * pre * (1.0 + tanh)).astype(BF16)
    hid_o[...] = hidden
    gd_o[...] = 0.5 * (1.0 + tanh) + 0.5 * pre * (1.0 - tanh * tanh) * (GC * (1.0 + 3.0 * GA * pre * pre))
    wfull[y, x, core] = w_proj[...]
    for j in range(2):
        cs[j] = dot(hidden, w_down[:, at((1 - core) * 2 + j, 512)]).astype(BF16)
    me.met()
    to_core = [send(cs.at[j], cr.at[j], me.other_core()) for j in range(2)]
    w_y = [send(w_proj, wfull.at[y, x, core], me.along_y(i)) for i in (1, 2, 3)]
    to_x = []
    for j in range(2):
        own = dot(hidden, w_down[:, at(core * 2 + j, 512)])
        to_core[j].wait_recv()
        xs[j] = (own + cr[j].astype(F32)).astype(BF16).reshape(4, 4, 16, 512)
        to_x.append(
            [send(xs.at[j, :, lax.rem(x + i, 4)], xr.at[j, i - 1], me.along_x(i)) for i in (2, 1, 3)]
        )
    for copy in w_y:
        copy.wait_recv()
    to_y = []
    for j in range(2):
        for copy in to_x[j]:
            copy.wait_recv()
        total = xs[j, :, x].astype(F32)
        for i in range(3):
            total += xr[j, i].astype(F32)
        ys[j] = total.astype(BF16)
        to_y.append([send(ys.at[j, lax.rem(y + i, 4)], yr.at[j, i - 1], me.along_y(i)) for i in (2, 1, 3)])
    w_x = [send(wfull.at[:, x, core], wfull.at[:, x, core], me.along_x(i)) for i in (1, 2, 3)]
    for j in range(2):
        for copy in to_y[j]:
            copy.wait_recv()
        total = ys[j, y].astype(F32)
        for i in range(3):
            total += yr[j, i].astype(F32)
        lo[core, :, j * 512 : (j + 1) * 512] = total
    half = send(lo.at[core], lo.at[core], me.other_core())
    for copy in w_x:
        copy.wait_recv()
    w_core = send(wfull.at[:, :, core], wfull.at[:, :, core], me.other_core())
    half.wait_recv()
    layer_out = tok[at(chip, 16), :].astype(F32) + jnp.concatenate([lo[0], lo[1]], axis=1)
    centred = layer_out - jnp.mean(layer_out, axis=1, keepdims=True)
    inv_scale = lax.rsqrt(jnp.mean(centred * centred, axis=1, keepdims=True) + EPS)
    out_hat = centred * inv_scale
    oh_o[...] = out_hat
    inv_o[...] = jnp.broadcast_to(inv_scale, (16, 128))
    final = out_hat * fgain[...]
    pooled = jnp.sum(final * pool_weights(plen, chip), axis=0, keepdims=True)
    pooled_low = pooled.astype(BF16)
    w_core.wait_recv()
    feat = dot(jnp.broadcast_to(pooled_low, (16, 2048)), wfull[...].reshape(2048, 256))
    frow[chip] = feat[:1].astype(BF16).astype(F32)
    to_plane = [send(frow.at[chip], frow.at[chip], me.in_plane(i)) for i in range(1, 16)]
    rounded = pooled_low.astype(F32)
    for k in range(16):
        psend[k] = rounded[:, k * 128 : (k + 1) * 128]
    prow[chip] = psend[chip]
    pooled_to = [send(psend.at[lax.rem(chip + i, 16)], prow.at[chip], me.in_plane(i)) for i in range(1, 16)]
    wfull_o[...] = wfull[...].reshape(2048, 256)
    for copy in to_plane:
        copy.wait_recv()
    allf[t] = jnp.concatenate([frow[k] for k in range(16)], axis=0).astype(BF16)
    to_text = [send(allf.at[t], allf.at[t], me.in_text(i)) for i in range(1, 16)]
    for copy in pooled_to:
        copy.wait_recv()
    pool_o[...] = jnp.concatenate([prow[k] for k in range(16)], axis=0).astype(BF16)
    for copy in to_text:
        copy.wait_recv()
    feat_o[...] = allf[...].reshape(256, 256)
    send.drain()


B_COPIES = 1 + 15 + 15 + 1 + 15 + 3 + 12 + 15 + 2 * 15


def backward_kernel(
    plen, ft, hid, nrm, gd, oh, inv, pool, wfull, w_down, fgain,
    up_o, down_o, proj_o,
    cs, cr, ts, tr, ps, pr, fgb, fgs, pj, pjf, og, h_t, n_t, ds, dyr, dz, dr, us, uyr, uz, ur,
    send_sems, recv_sems,
):
    me = Place()
    send = Sends(send_sems, recv_sems)
    core, chip, x, y, t, z, yl = me.core, me.chip, me.x, me.y, me.t, me.z, me.yl
    me.greet()
    cs[...] = ft[:, at(1 - core, 128)].astype(BF16)
    me.met()
    to_core = send(cs, cr, me.other_core())
    h_t[...] = hid[...].T
    to_core.wait_recv()
    ts[...] = (ft[:, at(core, 128)] + cr[...].astype(F32)).astype(BF16).reshape(16, 16, 128)
    to_text = [send(ts.at[lax.rem(t + i, 16)], tr.at[i - 1], me.in_text(i)) for i in range(1, 16)]
    n_t[...] = nrm[...].T
    total = ts[t].astype(F32)
    for i in range(15):
        to_text[i].wait_recv()
        total += tr[i].astype(F32)
    ps[...] = total
    to_plane = [send(ps, pr.at[i - 1], me.in_plane(i)) for i in range(1, 16)]
    for i in range(15):
        to_plane[i].wait_recv()
        total += pr[i]
    fgb[core] = total
    half = send(fgb.at[core], fgb.at[core], me.other_core())
    half.wait_recv()
    feat_grad = jnp.concatenate([fgb[0], fgb[1]], axis=1)
    fgs[...] = feat_grad
    row = fgs[pl.ds(chip, 1), :]
    high = row.astype(BF16).astype(F32)
    middle = (row - high).astype(BF16).astype(F32)
    low = row - high - middle
    part = lax.broadcasted_iota(jnp.int32, (16, 256), 0)
    rows = jnp.where(part == 0, high, jnp.where(part == 1, middle, jnp.where(part == 2, low, 0.0)))
    pooled_grad = jnp.sum(dot(rows.astype(BF16), wfull[...], ((1,), (1,))), axis=0, keepdims=True)
    hat = pooled_grad * fgain[...]
    out_hat = oh[...]
    first = jnp.mean(hat, axis=1, keepdims=True)
    second = jnp.mean(hat * out_hat, axis=1, keepdims=True)
    scale = pool_weights(plen, chip) * inv[:, :1]
    out_grad = ((hat - first - out_hat * second) * scale).astype(BF16)
    og[0, y, x] = out_grad[:, :1024]
    og[1, y, x] = out_grad[:, 1024:]
    mine = og.at[core, y, x]
    to_y = [send(mine, mine, me.along_y(i)) for i in (2, 1, 3)]
    waves = [[send(mine, mine, me.along_x(i)) for i in (2, 1, 3)]]
    pj[t, :, :256] = feat_grad.astype(BF16)
    pj[t, :, 256:] = pool[...]
    to_other = []
    pj_to = [send(pj.at[t], pj.at[t], me.in_text(i)) for i in range(1, 16)]
    for copy, i in ((to_y[1], 1), (to_y[2], 3), (to_y[0], 2)):
        copy.wait_recv()
        block = og.at[core, lax.rem(y + 4 - i, 4), x]
        waves.append([send(block, block, me.along_x(j)) for j in (2, 1, 3)])
        to_other.append(send(block, block, me.other_core()))
    for wave, i in zip(waves, (0, 1, 3, 2)):
        for copy, j in zip(wave, (2, 1, 3)):
            copy.wait_recv()
            block = og.at[core, lax.rem(y + 4 - i, 4), lax.rem(x + 4 - j, 4)]
            to_other.append(send(block, block, me.other_core()))
    for copy in to_other:
        copy.wait_recv()
    order = (4, 3, 5, 2, 6, 1, 7, 0)

    def exchange(parts, arrived):
        copies = {}
        for i in order:
            spot = lax.rem(z + i, 8)
            copies[i] = send(parts.at[spot, 1 - yl], arrived.at[i], me.across())
        return copies

    def onward(copies, parts, arrived, staged, landed):
        copies_z = {}
        for i in order[:-1]:
            copies[i].wait_recv()
            staged[i - 1] = (parts[lax.rem(z + i, 8), yl].astype(F32) + arrived[i].astype(F32)).astype(BF16)
            copies_z[i] = send(staged.at[i - 1], landed.at[i - 1], me.along_z(i))
        return copies_z

    def finish(copies, copies_z, parts, arrived, landed, out):
        copies[0].wait_recv()
        total = parts[z, yl].astype(F32) + arrived[0].astype(F32)
        for i in (1, 7, 2, 6, 3, 5, 4):
            copies_z[i].wait_recv()
            total += landed[i - 1].astype(F32)
        out[...] = total

    halves = [og[h].reshape(256, 1024) for h in range(2)]
    for h in range(2):
        product = dot(h_t[...], halves[h]).astype(BF16)
        for k in range(8):
            ds[h * 4 + k // 2, k % 2] = product[:, k * 128 : (k + 1) * 128]
    down_y = exchange(ds, dyr)
    hidden_grad = dot(halves[0], w_down[:, :1024], ((1,), (1,))) + dot(halves[1], w_down[:, 1024:], ((1,), (1,)))
    pre_grad = (hidden_grad * gd[...]).astype(BF16)
    us[...] = dot(n_t[...], pre_grad).astype(BF16).reshape(8, 2, 128, 256)
    up_y = exchange(us, uyr)
    down_z = onward(down_y, ds, dyr, dz, dr)
    up_z = onward(up_y, us, uyr, uz, ur)
    for copy in pj_to:
        copy.wait_recv()
    pjf[...] = dot(pj[:, :, 256:].reshape(256, 128), pj[:, :, :256].reshape(256, 256), ((0,), (0,)))
    proj_o[...] = pjf[at(core, 64), :]
    finish(down_y, down_z, ds, dyr, dr, down_o)
    finish(up_y, up_z, us, uyr, ur, up_o)
    send.drain()


def vmem(n):
    return [pl.BlockSpec(memory_space=pltpu.VMEM)] * n


def forward(plen, tok, ngain, w_up, w_down, fgain, w_proj):
    return pl.pallas_call(
        forward_kernel,
        name="forward",
        in_specs=[pl.BlockSpec(memory_space=pltpu.SMEM)] + vmem(6),
        out_specs=vmem(8),
        out_shape=(
            jax.ShapeDtypeStruct((256, 256), BF16),
            jax.ShapeDtypeStruct((256, 256), BF16),
            jax.ShapeDtypeStruct((256, 2048), BF16),
            jax.ShapeDtypeStruct((256, 256), F32),
            jax.ShapeDtypeStruct((16, 2048), F32),
            jax.ShapeDtypeStruct((16, 128), F32),
            jax.ShapeDtypeStruct((16, 128), BF16),
            jax.ShapeDtypeStruct((2048, 256), BF16),
        ),
        scratch_shapes=[
            pltpu.VMEM((2, 256, 512), BF16),
            pltpu.VMEM((2, 256, 512), BF16),
            pltpu.VMEM((2, 4, 4, 16, 512), BF16),
            pltpu.VMEM((2, 3, 4, 16, 512), BF16),
            pltpu.VMEM((2, 4, 16, 512), BF16),
            pltpu.VMEM((2, 3, 16, 512), BF16),
            pltpu.VMEM((2, 16, 1024), F32),
            pltpu.VMEM((4, 4, 2, 64, 256), BF16),
            pltpu.VMEM((16, 1, 256), F32),
            pltpu.VMEM((16, 1, 128), F32),
            pltpu.VMEM((16, 1, 128), F32),
            pltpu.VMEM((16, 16, 256), BF16),
            pltpu.SemaphoreType.DMA((A_COPIES,)),
            pltpu.SemaphoreType.DMA((A_COPIES,)),
        ],
        compiler_params=pltpu.CompilerParams(
            collective_id=0, has_side_effects=True, vmem_limit_bytes=40 << 20
        ),
    )(plen, tok, ngain, w_up, w_down, fgain, w_proj)


def backward(plen, ft, hid, nrm, gd, oh, inv, pool, wfull, w_down, fgain):
    return pl.pallas_call(
        backward_kernel,
        name="backward",
        in_specs=[pl.BlockSpec(memory_space=pltpu.SMEM)] + vmem(10),
        out_specs=vmem(3),
        out_shape=(
            jax.ShapeDtypeStruct((128, 256), F32),
            jax.ShapeDtypeStruct((256, 128), F32),
            jax.ShapeDtypeStruct((64, 256), F32),
        ),
        scratch_shapes=[
            pltpu.VMEM((256, 128), BF16),
            pltpu.VMEM((256, 128), BF16),
            pltpu.VMEM((16, 16, 128), BF16),
            pltpu.VMEM((15, 16, 128), BF16),
            pltpu.VMEM((16, 128), F32),
            pltpu.VMEM((15, 16, 128), F32),
            pltpu.VMEM((2, 16, 128), F32),
            pltpu.VMEM((16, 256), F32),
            pltpu.VMEM((16, 16, 384), BF16),
            pltpu.VMEM((128, 256), F32),
            pltpu.VMEM((2, 4, 4, 16, 1024), BF16),
            pltpu.VMEM((256, 256), BF16),
            pltpu.VMEM((2048, 256), BF16),
            pltpu.VMEM((8, 2, 256, 128), BF16),
            pltpu.VMEM((8, 256, 128), BF16),
            pltpu.VMEM((7, 256, 128), BF16),
            pltpu.VMEM((7, 256, 128), BF16),
            pltpu.VMEM((8, 2, 128, 256), BF16),
            pltpu.VMEM((8, 128, 256), BF16),
            pltpu.VMEM((7, 128, 256), BF16),
            pltpu.VMEM((7, 128, 256), BF16),
            pltpu.SemaphoreType.DMA((B_COPIES,)),
            pltpu.SemaphoreType.DMA((B_COPIES,)),
        ],
        compiler_params=pltpu.CompilerParams(
            collective_id=1, has_side_effects=True, vmem_limit_bytes=40 << 20
        ),
    )(plen, ft, hid, nrm, gd, oh, inv, pool, wfull, w_down, fgain)


def focal_total(scores, target, weight):
    log_pos = jax.nn.log_sigmoid(scores)
    log_neg = jax.nn.log_sigmoid(-scores)
    probab = jax.nn.sigmoid(scores)
    pos_term = -ALPHA * target * (1.0 - probab) ** 2 * log_pos
    neg_term = -(1.0 - ALPHA) * (1.0 - target) * probab**2 * log_neg
    return jnp.sum(weight * (pos_term + neg_term))


def body(
    prompt_embeds, prompt_len, norm_gain, w_up, w_down, final_gain, w_proj, queries, assign, valid
):
    tok = prompt_embeds.reshape(256, 2048)
    ngain, fgain = norm_gain.reshape(1, 2048), final_gain.reshape(1, 2048)
    all_feat, hid, nrm, gd, oh, inv, pool, wfull = forward(
        prompt_len, tok, ngain, w_up, w_down, fgain, w_proj
    )
    img_count, query_count, query_width = queries.shape
    query_rows = img_count * query_count
    concept_count = all_feat.shape[0]
    flat_queries = queries.reshape(query_rows, query_width)
    score_scale = query_width ** (-0.5)
    scores = dot(flat_queries, all_feat, ((1,), (1,))) * score_scale + LOGIT_BIAS
    column = lax.broadcasted_iota(jnp.int32, (img_count, query_count, concept_count), 2)
    target = (assign[:, :, None] == column).astype(F32).reshape(query_rows, concept_count)
    weight = jnp.broadcast_to(
        valid[:, None, :].astype(F32), (img_count, query_count, concept_count)
    ).reshape(query_rows, concept_count)
    score_grad = jax.grad(focal_total)(scores, target, weight).astype(BF16)
    query_grad = dot(score_grad, all_feat) * score_scale
    images = img_count * lax.axis_size("text") * lax.axis_size("det")
    feat_terms = dot(score_grad, flat_queries, ((0,), (0,))) * (score_scale / images)
    up_grad, down_grad, proj_grad = backward(
        prompt_len, feat_terms, hid, nrm, gd, oh, inv, pool, wfull, w_down, fgain
    )
    return (up_grad, down_grad, proj_grad, query_grad.reshape(img_count, query_count, query_width))


def solution(mesh):
    return jax.shard_map(
        body,
        mesh=mesh,
        in_specs=(
            P("text", None, None),
            P("text"),
            P(),
            P(None, "det"),
            P("det", None),
            P(),
            P("det", None),
            P(("text", "det"), None, None),
            P(("text", "det"), None),
            P(("text", "det"), None),
        ),
        out_specs=(
            P("text", "det"),
            P("det", "text"),
            P("det", None),
            P(("text", "det"), None, None),
        ),
        check_vma=False,
    )
```

```python
import jax
import jax.numpy as jnp
from jax import lax
from jax.experimental import pallas as pl
from jax.experimental.pallas import tpu as pltpu
from jax.sharding import PartitionSpec as P

EPS = 1e-05
ALPHA = 0.25
LOGIT_BIAS = -2.0
F32 = jnp.float32
BF16 = jnp.bfloat16
MESH = pl.DeviceIdType.MESH
GC = 0.7978845608028654
GA = 0.044715


class Place:
    def __init__(self):
        self.t = lax.axis_index("text")
        self.d = lax.axis_index("det")
        self.core = lax.rem(self.d, 2)
        self.chip = self.d // 2
        self.x = lax.rem(self.chip, 4)
        self.y = self.chip // 4
        self.z = self.t // 2
        self.yl = lax.rem(self.t, 2)

    def other_core(self):
        return {"det": self.d + 1 - 2 * self.core}

    def along_x(self, i):
        return {"det": (self.y * 4 + lax.rem(self.x + i, 4)) * 2 + self.core}

    def along_y(self, i):
        return {"det": (lax.rem(self.y + i, 4) * 4 + self.x) * 2 + self.core}

    def in_plane(self, i, swap=0):
        core = 1 - self.core if swap else self.core
        return {"det": lax.rem(self.chip + i, 16) * 2 + core}

    def in_text(self, i):
        return {"text": lax.rem(self.t + i, 16)}

    def along_z(self, i):
        return {"text": lax.rem(self.z + i, 8) * 2 + self.yl}

    def across(self):
        return {"text": self.t + 1 - 2 * self.yl}

    def greet(self):
        barrier = pltpu.get_barrier_semaphore()
        pl.semaphore_signal(barrier, inc=1, device_id=self.other_core(), device_id_type=MESH)
        for i in range(1, 16):
            pl.semaphore_signal(barrier, inc=1, device_id=self.in_plane(i), device_id_type=MESH)
            pl.semaphore_signal(barrier, inc=1, device_id=self.in_plane(i, 1), device_id_type=MESH)
            pl.semaphore_signal(barrier, inc=1, device_id=self.in_text(i), device_id_type=MESH)

    def met(self):
        pl.semaphore_wait(pltpu.get_barrier_semaphore(), 46)


class Sends:
    def __init__(self, send_sems, recv_sems):
        self.send_sems, self.recv_sems, self.used = send_sems, recv_sems, 0
        self.flying = []

    def __call__(self, src, dst, to):
        copy = pltpu.make_async_remote_copy(
            src_ref=src,
            dst_ref=dst,
            send_sem=self.send_sems.at[self.used],
            recv_sem=self.recv_sems.at[self.used],
            device_id=to,
            device_id_type=MESH,
        )
        self.used += 1
        copy.start()
        self.flying.append(copy)
        return copy

    def drain(self):
        for copy in self.flying:
            copy.wait_send()


def at(i, n):
    return pl.ds(pl.multiple_of(i * n, n), n)


def dot(a, b, dims=((1,), (0,))):
    return lax.dot_general(a, b, (dims, ((), ())), preferred_element_type=F32)


def pool_weights(plen, chip):
    lane = lax.broadcasted_iota(jnp.int32, (16, 16), 1)
    length = jnp.sum(jnp.where(lane == chip, plen[...], 0).astype(F32), axis=1, keepdims=True)
    slot = lax.broadcasted_iota(jnp.int32, (16, 1), 0).astype(F32)
    return jnp.where(slot < length, 1.0 / length, 0.0)


COPIES = 2 + 3 + 6 + 6 + 3 + 1 + 1 + 15 + 15 + 15 + 1 + 15 + 31 + 15 + 15 + 3 + 12 + 15 + 30
SCORE_SCALE = 256 ** (-0.5)
IMAGES = 512


def step_kernel(
    plen_h, tok_h, ngain_h, w_up_h, w_down_h, fgain_h, w_proj_h, quer_h, assign_h, valid_h,
    up_h, down_h, proj_h, qg_h,
    plen, tok, ngain, w_up, w_down, fgain, w_proj, quer, assign, valid,
    nrm, gd, cs, cr, xs, xr, ys, yr, lo, wfull, frow, psend, prow, allf, vcol, score, sgrad, qg,
    fcs, fcr, ts, tr, rsend, rgot, grow, pj, pjf, og, h_t, n_t,
    ds, dyr, dz, dr, us, uyr, uz, ur, up_v, down_v, proj_v,
    load_sems, store_sems, send_sems, recv_sems,
):
    me = Place()
    send = Sends(send_sems, recv_sems)
    core, chip, x, y, t, z, yl = me.core, me.chip, me.x, me.y, me.t, me.z, me.yl
    me.greet()
    loads = {}
    for n, (name, src, dst) in enumerate((
        ("tok", tok_h, tok), ("ngain", ngain_h, ngain), ("w_up", w_up_h, w_up), ("w_down", w_down_h, w_down),
        ("w_proj", w_proj_h, w_proj), ("plen", plen_h, plen), ("fgain", fgain_h, fgain),
        ("quer", quer_h, quer), ("assign", assign_h, assign), ("valid", valid_h, valid),
    )):
        loads[name] = pltpu.make_async_copy(src, dst, load_sems.at[n])
        loads[name].start()
    stores = []

    def store(src, dst):
        copy = pltpu.make_async_copy(src, dst, store_sems.at[len(stores)])
        copy.start()
        stores.append(copy)

    loads["tok"].wait()
    loads["ngain"].wait()
    tokens = tok[...].astype(F32)
    centred = tokens - jnp.mean(tokens, axis=1, keepdims=True)
    variance = jnp.mean(centred * centred, axis=1, keepdims=True)
    normed = (centred * lax.rsqrt(variance + EPS) * ngain[...]).astype(BF16)
    nrm[...] = normed
    loads["w_up"].wait()
    pre = dot(normed, w_up[...])
    tanh = jnp.tanh(GC * (pre + GA * pre * pre * pre))
    hidden = (0.5 * pre * (1.0 + tanh)).astype(BF16)
    gd[...] = 0.5 * (1.0 + tanh) + 0.5 * pre * (1.0 - tanh * tanh) * (GC * (1.0 + 3.0 * GA * pre * pre))
    loads["w_proj"].wait()
    loads["w_down"].wait()
    wfull[y, x, core] = w_proj[...]
    for j in range(2):
        cs[j] = dot(hidden, w_down[:, at((1 - core) * 2 + j, 512)]).astype(BF16)
    me.met()
    to_core = [send(cs.at[j], cr.at[j], me.other_core()) for j in range(2)]
    w_y = [send(w_proj, wfull.at[y, x, core], me.along_y(i)) for i in (1, 2, 3)]
    to_x = []
    for j in range(2):
        own = dot(hidden, w_down[:, at(core * 2 + j, 512)])
        to_core[j].wait_recv()
        xs[j] = (own + cr[j].astype(F32)).astype(BF16).reshape(4, 4, 16, 512)
        to_x.append(
            [send(xs.at[j, :, lax.rem(x + i, 4)], xr.at[j, i - 1], me.along_x(i)) for i in (2, 1, 3)]
        )
    h_t[...] = hidden.T
    for name in ("plen", "fgain", "quer", "assign", "valid"):
        loads[name].wait()
    vcol[...] = jnp.broadcast_to(valid[...].astype(F32), (128, 256)).T
    for copy in w_y:
        copy.wait_recv()
    to_y = []
    for j in range(2):
        for copy in to_x[j]:
            copy.wait_recv()
        total = xs[j, :, x].astype(F32)
        for i in range(3):
            total += xr[j, i].astype(F32)
        ys[j] = total.astype(BF16)
        to_y.append([send(ys.at[j, lax.rem(y + i, 4)], yr.at[j, i - 1], me.along_y(i)) for i in (2, 1, 3)])
    w_x = [send(wfull.at[:, x, core], wfull.at[:, x, core], me.along_x(i)) for i in (1, 2, 3)]
    for j in range(2):
        for copy in to_y[j]:
            copy.wait_recv()
        total = ys[j, y].astype(F32)
        for i in range(3):
            total += yr[j, i].astype(F32)
        lo[core, :, j * 512 : (j + 1) * 512] = total
    half = send(lo.at[core], lo.at[core], me.other_core())
    for copy in w_x:
        copy.wait_recv()
    w_core = send(wfull.at[:, :, core], wfull.at[:, :, core], me.other_core())
    half.wait_recv()
    layer_out = tok[at(chip, 16), :].astype(F32) + jnp.concatenate([lo[0], lo[1]], axis=1)
    centred = layer_out - jnp.mean(layer_out, axis=1, keepdims=True)
    inv_scale = lax.rsqrt(jnp.mean(centred * centred, axis=1, keepdims=True) + EPS)
    out_hat = centred * inv_scale
    final = out_hat * fgain[...]
    pool_weight = pool_weights(plen, chip)
    pooled = jnp.sum(final * pool_weight, axis=0, keepdims=True)
    pooled_low = pooled.astype(BF16)
    w_core.wait_recv()
    feat = dot(jnp.broadcast_to(pooled_low, (16, 2048)), wfull[...].reshape(2048, 256))
    frow[chip] = feat[:1].astype(BF16).astype(F32)
    to_plane = [send(frow.at[chip], frow.at[chip], me.in_plane(i)) for i in range(1, 16)]
    rounded = pooled_low.astype(F32)
    for k in range(16):
        psend[k] = rounded[:, k * 128 : (k + 1) * 128]
    prow[chip] = psend[chip]
    pooled_to = [send(psend.at[lax.rem(chip + i, 16)], prow.at[chip], me.in_plane(i)) for i in range(1, 16)]
    n_t[...] = nrm[...].T
    for copy in to_plane:
        copy.wait_recv()
    allf[t] = jnp.concatenate([frow[k] for k in range(16)], axis=0).astype(BF16)
    to_text = [send(allf.at[t], allf.at[t], me.in_text(i)) for i in range(1, 16)]
    for copy in pooled_to:
        copy.wait_recv()
    pj[t, :, 256:] = jnp.concatenate([prow[k] for k in range(16)], axis=0).astype(BF16)
    for copy in to_text:
        copy.wait_recv()

    features = allf[...].reshape(256, 256)
    score[...] = dot(features, quer[...], ((1,), (1,)))
    chosen = assign[...]

    @pl.loop(0, 16)
    def _(r):
        spot = at(r, 16)
        s = score[spot, :] * SCORE_SCALE + LOGIT_BIAS
        concept = lax.broadcasted_iota(jnp.int32, (16, 1100), 0) + r * 16
        hit = concept == chosen
        u = jnp.where(hit, -s, s)
        e = jnp.exp(-jnp.abs(u))
        more = 1.0 / (1.0 + e)
        less = e * more
        p = jnp.where(u >= 0.0, more, less)
        q = jnp.where(u >= 0.0, less, more)
        soft = jnp.maximum(u, 0.0) + jnp.log1p(e)
        factor = jnp.where(hit, -ALPHA, 1.0 - ALPHA) * vcol[spot, :1]
        sgrad[spot, :] = (factor * p * p * (p + 2.0 * q * soft)).astype(BF16)

    terms = dot(sgrad[...], quer[...]) * (SCORE_SCALE / IMAGES)
    halves = (terms[:, :128], terms[:, 128:])
    mine = jnp.where(core == 0, halves[0], halves[1])
    fcs[...] = jnp.where(core == 0, halves[1], halves[0]).astype(BF16)
    to_core = send(fcs, fcr, me.other_core())
    to_core.wait_recv()
    ts[...] = (mine + fcr[...].astype(F32)).astype(BF16).reshape(16, 16, 128)
    to_text2 = [send(ts.at[lax.rem(t + i, 16)], tr.at[i - 1], me.in_text(i)) for i in range(1, 16)]
    query_grad = dot(sgrad[...], features, ((0,), (0,))) * SCORE_SCALE
    qg[pl.ds(0, 1100, stride=2), :] = query_grad[:, :128]
    qg[pl.ds(1, 1100, stride=2), :] = query_grad[:, 128:]
    store(qg, qg_h)
    total = ts[t].astype(F32)
    for i in range(15):
        to_text2[i].wait_recv()
        total += tr[i].astype(F32)
    for k in range(16):
        rsend[k] = total[k : k + 1]
    rgot[core, chip] = rsend[chip]
    to_rows = [send(rsend.at[chip], rgot.at[core, chip], me.other_core())]
    for i in range(1, 16):
        there = rsend.at[lax.rem(chip + i, 16)]
        to_rows.append(send(there, rgot.at[core, chip], me.in_plane(i)))
        to_rows.append(send(there, rgot.at[core, chip], me.in_plane(i, 1)))
    for copy in to_rows:
        copy.wait_recv()
    sums = []
    for c in range(2):
        total = rgot[c, 0]
        for k in range(1, 16):
            total += rgot[c, k]
        sums.append(total)
    row = jnp.concatenate(sums, axis=1)
    grow[chip] = row
    high = row.astype(BF16).astype(F32)
    middle = (row - high).astype(BF16).astype(F32)
    low = row - high - middle
    part = lax.broadcasted_iota(jnp.int32, (16, 256), 0)
    rows = jnp.where(part == 0, high, jnp.where(part == 1, middle, jnp.where(part == 2, low, 0.0)))
    pooled_grad = jnp.sum(
        dot(rows.astype(BF16), wfull[...].reshape(2048, 256), ((1,), (1,))), axis=0, keepdims=True
    )
    hat = pooled_grad * fgain[...]
    first = jnp.mean(hat, axis=1, keepdims=True)
    second = jnp.mean(hat * out_hat, axis=1, keepdims=True)
    out_grad = ((hat - first - out_hat * second) * (pool_weight * inv_scale)).astype(BF16)
    og[0, y, x] = out_grad[:, :1024]
    og[1, y, x] = out_grad[:, 1024:]
    own = og.at[core, y, x]
    to_y = [send(own, own, me.along_y(i)) for i in (2, 1, 3)]
    waves = [[send(own, own, me.along_x(i)) for i in (2, 1, 3)]]
    to_grow = [send(grow.at[chip], grow.at[chip], me.in_plane(i)) for i in range(1, 16)]
    to_other = []
    for copy, i in ((to_y[1], 1), (to_y[2], 3), (to_y[0], 2)):
        copy.wait_recv()
        block = og.at[core, lax.rem(y + 4 - i, 4), x]
        waves.append([send(block, block, me.along_x(j)) for j in (2, 1, 3)])
        to_other.append(send(block, block, me.other_core()))
    for copy in to_grow:
        copy.wait_recv()
    pj[t, :, :256] = jnp.concatenate([grow[k] for k in range(16)], axis=0).astype(BF16)
    pj_to = [send(pj.at[t], pj.at[t], me.in_text(i)) for i in range(1, 16)]
    for wave, i in zip(waves, (0, 1, 3, 2)):
        for copy, j in zip(wave, (2, 1, 3)):
            copy.wait_recv()
            block = og.at[core, lax.rem(y + 4 - i, 4), lax.rem(x + 4 - j, 4)]
            to_other.append(send(block, block, me.other_core()))
    for copy in to_other:
        copy.wait_recv()
    order = (4, 3, 5, 2, 6, 1, 7, 0)

    def exchange(parts, arrived):
        copies = {}
        for i in order:
            spot = lax.rem(z + i, 8)
            copies[i] = send(parts.at[spot, 1 - yl], arrived.at[i], me.across())
        return copies

    def onward(copies, parts, arrived, staged, landed):
        copies_z = {}
        for i in order[:-1]:
            copies[i].wait_recv()
            staged[i - 1] = (parts[lax.rem(z + i, 8), yl].astype(F32) + arrived[i].astype(F32)).astype(BF16)
            copies_z[i] = send(staged.at[i - 1], landed.at[i - 1], me.along_z(i))
        return copies_z

    def finish(copies, copies_z, parts, arrived, landed, out):
        copies[0].wait_recv()
        total = parts[z, yl].astype(F32) + arrived[0].astype(F32)
        for i in (1, 7, 2, 6, 3, 5, 4):
            copies_z[i].wait_recv()
            total += landed[i - 1].astype(F32)
        out[...] = total

    halves = [og[h].reshape(256, 1024) for h in range(2)]
    for h in range(2):
        product = dot(h_t[...], halves[h]).astype(BF16)
        for k in range(8):
            ds[h * 4 + k // 2, k % 2] = product[:, k * 128 : (k + 1) * 128]
    down_y = exchange(ds, dyr)
    hidden_grad = dot(halves[0], w_down[:, :1024], ((1,), (1,))) + dot(halves[1], w_down[:, 1024:], ((1,), (1,)))
    pre_grad = (hidden_grad * gd[...]).astype(BF16)
    us[...] = dot(n_t[...], pre_grad).astype(BF16).reshape(8, 2, 128, 256)
    up_y = exchange(us, uyr)
    down_z = onward(down_y, ds, dyr, dz, dr)
    up_z = onward(up_y, us, uyr, uz, ur)
    for copy in pj_to:
        copy.wait_recv()
    pjf[...] = dot(pj[:, :, 256:].reshape(256, 128), pj[:, :, :256].reshape(256, 256), ((0,), (0,)))
    proj_v[...] = pjf[at(core, 64), :]
    store(proj_v, proj_h)
    finish(down_y, down_z, ds, dyr, dr, down_v)
    store(down_v, down_h)
    finish(up_y, up_z, us, uyr, ur, up_v)
    store(up_v, up_h)
    send.drain()
    for copy in stores:
        copy.wait()


def step(*args):
    anywhere = pl.BlockSpec(memory_space=pl.ANY)
    return pl.pallas_call(
        step_kernel,
        name="step",
        in_specs=[anywhere] * 10,
        out_specs=[anywhere] * 4,
        out_shape=(
            jax.ShapeDtypeStruct((128, 256), F32),
            jax.ShapeDtypeStruct((256, 128), F32),
            jax.ShapeDtypeStruct((64, 256), F32),
            jax.ShapeDtypeStruct((2200, 128), F32),
        ),
        scratch_shapes=[
            pltpu.VMEM((1, 16), jnp.int32),
            pltpu.VMEM((256, 2048), BF16),
            pltpu.VMEM((1, 2048), F32),
            pltpu.VMEM((2048, 256), BF16),
            pltpu.VMEM((256, 2048), BF16),
            pltpu.VMEM((1, 2048), F32),
            pltpu.VMEM((64, 256), BF16),
            pltpu.VMEM((1100, 256), BF16),
            pltpu.VMEM((1, 1100), jnp.int32),
            pltpu.VMEM((1, 256), jnp.int32),
            pltpu.VMEM((256, 2048), BF16),
            pltpu.VMEM((256, 256), F32),
            pltpu.VMEM((2, 256, 512), BF16),
            pltpu.VMEM((2, 256, 512), BF16),
            pltpu.VMEM((2, 4, 4, 16, 512), BF16),
            pltpu.VMEM((2, 3, 4, 16, 512), BF16),
            pltpu.VMEM((2, 4, 16, 512), BF16),
            pltpu.VMEM((2, 3, 16, 512), BF16),
            pltpu.VMEM((2, 16, 1024), F32),
            pltpu.VMEM((4, 4, 2, 64, 256), BF16),
            pltpu.VMEM((16, 1, 256), F32),
            pltpu.VMEM((16, 1, 128), F32),
            pltpu.VMEM((16, 1, 128), F32),
            pltpu.VMEM((16, 16, 256), BF16),
            pltpu.VMEM((256, 128), F32),
            pltpu.VMEM((256, 1100), F32),
            pltpu.VMEM((256, 1100), BF16),
            pltpu.VMEM((2200, 128), F32),
            pltpu.VMEM((256, 128), BF16),
            pltpu.VMEM((256, 128), BF16),
            pltpu.VMEM((16, 16, 128), BF16),
            pltpu.VMEM((15, 16, 128), BF16),
            pltpu.VMEM((16, 1, 128), F32),
            pltpu.VMEM((2, 16, 1, 128), F32),
            pltpu.VMEM((16, 1, 256), F32),
            pltpu.VMEM((16, 16, 384), BF16),
            pltpu.VMEM((128, 256), F32),
            pltpu.VMEM((2, 4, 4, 16, 1024), BF16),
            pltpu.VMEM((256, 256), BF16),
            pltpu.VMEM((2048, 256), BF16),
            pltpu.VMEM((8, 2, 256, 128), BF16),
            pltpu.VMEM((8, 256, 128), BF16),
            pltpu.VMEM((7, 256, 128), BF16),
            pltpu.VMEM((7, 256, 128), BF16),
            pltpu.VMEM((8, 2, 128, 256), BF16),
            pltpu.VMEM((8, 128, 256), BF16),
            pltpu.VMEM((7, 128, 256), BF16),
            pltpu.VMEM((7, 128, 256), BF16),
            pltpu.VMEM((128, 256), F32),
            pltpu.VMEM((256, 128), F32),
            pltpu.VMEM((64, 256), F32),
            pltpu.SemaphoreType.DMA((10,)),
            pltpu.SemaphoreType.DMA((4,)),
            pltpu.SemaphoreType.DMA((COPIES,)),
            pltpu.SemaphoreType.DMA((COPIES,)),
        ],
        compiler_params=pltpu.CompilerParams(
            collective_id=0, has_side_effects=True, vmem_limit_bytes=62 << 20
        ),
    )(*args)


def body(
    prompt_embeds, prompt_len, norm_gain, w_up, w_down, final_gain, w_proj, queries, assign, valid
):
    up_grad, down_grad, proj_grad, query_grad = step(
        prompt_len.reshape(1, 16),
        prompt_embeds.reshape(256, 2048),
        norm_gain.reshape(1, 2048),
        w_up,
        w_down,
        final_gain.reshape(1, 2048),
        w_proj,
        queries.reshape(1100, 256),
        assign,
        valid,
    )
    return (up_grad, down_grad, proj_grad, query_grad.reshape(1, 1100, 256))


def solution(mesh):
    return jax.shard_map(
        body,
        mesh=mesh,
        in_specs=(
            P("text", None, None),
            P("text"),
            P(),
            P(None, "det"),
            P("det", None),
            P(),
            P("det", None),
            P(("text", "det"), None, None),
            P(("text", "det"), None),
            P(("text", "det"), None),
        ),
        out_specs=(
            P("text", "det"),
            P("det", "text"),
            P("det", None),
            P(("text", "det"), None, None),
        ),
        check_vma=False,
    )
```

```python
import jax
import jax.numpy as jnp
from jax import lax
from jax.experimental import pallas as pl
from jax.experimental.pallas import tpu as pltpu
from jax.sharding import PartitionSpec as P

EPS = 1e-05
ALPHA = 0.25
LOGIT_BIAS = -2.0
F32 = jnp.float32
BF16 = jnp.bfloat16
MESH = pl.DeviceIdType.MESH
GC = 0.7978845608028654
GA = 0.044715


class Place:
    def __init__(self):
        self.t = lax.axis_index("text")
        self.d = lax.axis_index("det")
        self.core = lax.rem(self.d, 2)
        self.chip = self.d // 2
        self.x = lax.rem(self.chip, 4)
        self.y = self.chip // 4
        self.z = self.t // 2
        self.yl = lax.rem(self.t, 2)

    def other_core(self):
        return {"det": self.d + 1 - 2 * self.core}

    def along_x(self, i):
        return {"det": (self.y * 4 + lax.rem(self.x + i, 4)) * 2 + self.core}

    def along_y(self, i):
        return {"det": (lax.rem(self.y + i, 4) * 4 + self.x) * 2 + self.core}

    def in_plane(self, i, swap=0):
        core = 1 - self.core if swap else self.core
        return {"det": lax.rem(self.chip + i, 16) * 2 + core}

    def in_text(self, i):
        return {"text": lax.rem(self.t + i, 16)}

    def along_z(self, i):
        return {"text": lax.rem(self.z + i, 8) * 2 + self.yl}

    def across(self):
        return {"text": self.t + 1 - 2 * self.yl}

    def greet(self):
        barrier = pltpu.get_barrier_semaphore()
        pl.semaphore_signal(barrier, inc=1, device_id=self.other_core(), device_id_type=MESH)
        for i in range(1, 16):
            pl.semaphore_signal(barrier, inc=1, device_id=self.in_plane(i), device_id_type=MESH)
            pl.semaphore_signal(barrier, inc=1, device_id=self.in_plane(i, 1), device_id_type=MESH)
            pl.semaphore_signal(barrier, inc=1, device_id=self.in_text(i), device_id_type=MESH)

    def met(self):
        pl.semaphore_wait(pltpu.get_barrier_semaphore(), 46)


class Sends:
    def __init__(self, send_sems, recv_sems):
        self.send_sems, self.recv_sems, self.used = send_sems, recv_sems, 0
        self.flying = []

    def __call__(self, src, dst, to):
        copy = pltpu.make_async_remote_copy(
            src_ref=src,
            dst_ref=dst,
            send_sem=self.send_sems.at[self.used],
            recv_sem=self.recv_sems.at[self.used],
            device_id=to,
            device_id_type=MESH,
        )
        self.used += 1
        copy.start()
        self.flying.append(copy)
        return copy

    def drain(self):
        for copy in self.flying:
            copy.wait_send()


def at(i, n):
    return pl.ds(pl.multiple_of(i * n, n), n)


def dot(a, b, dims=((1,), (0,))):
    return lax.dot_general(a, b, (dims, ((), ())), preferred_element_type=F32)


def pool_weights(plen, chip):
    lane = lax.broadcasted_iota(jnp.int32, (16, 16), 1)
    length = jnp.sum(jnp.where(lane == chip, plen[...], 0).astype(F32), axis=1, keepdims=True)
    slot = lax.broadcasted_iota(jnp.int32, (16, 1), 0).astype(F32)
    return jnp.where(slot < length, 1.0 / length, 0.0)


COPIES = 2 + 3 + 6 + 6 + 3 + 1 + 1 + 15 + 15 + 15 + 1 + 15 + 31 + 15 + 15 + 3 + 12 + 15 + 15 + 7 + 7 + 3 + 12 + 16 + 1
SCORE_SCALE = 256 ** (-0.5)
IMAGES = 512


def step_kernel(
    plen_h, tok_h, ngain_h, w_up_h, w_down_h, fgain_h, w_proj_h, quer_h, assign_h, valid_h,
    up_h, down_h, proj_h, qg_h,
    plen, tok, ngain, w_up, w_down, fgain, w_proj, quer, assign, valid,
    nrm, gd, cs, cr, xs, xr, ys, yr, lo, wfull, frow, psend, prow, allf, vcol, score, sgrad, qg, up_o, down_o, proj_o,
    fcs, fcr, ts, tr, rsend, rgot, grow, pj, pjf, og, h_all, n_t, ogz, dg, dp, dpr,
    us, uyr, uz, ur, load_sems, store_sems, send_sems, recv_sems,
):
    me = Place()
    send = Sends(send_sems, recv_sems)
    core, chip, x, y, t, z, yl = me.core, me.chip, me.x, me.y, me.t, me.z, me.yl
    me.greet()
    loads = {}
    for n, (name, src, dst) in enumerate((
        ("tok", tok_h, tok), ("ngain", ngain_h, ngain), ("w_up", w_up_h, w_up), ("w_down", w_down_h, w_down),
        ("w_proj", w_proj_h, w_proj), ("plen", plen_h, plen), ("fgain", fgain_h, fgain),
        ("quer", quer_h, quer), ("assign", assign_h, assign), ("valid", valid_h, valid),
    )):
        loads[name] = pltpu.make_async_copy(src, dst, load_sems.at[n])
        loads[name].start()
    stores = []

    def store(src, dst):
        copy = pltpu.make_async_copy(src, dst, store_sems.at[len(stores)])
        copy.start()
        stores.append(copy)

    loads["tok"].wait()
    loads["ngain"].wait()
    tokens = tok[...].astype(F32)
    centred = tokens - jnp.mean(tokens, axis=1, keepdims=True)
    variance = jnp.mean(centred * centred, axis=1, keepdims=True)
    normed = (centred * lax.rsqrt(variance + EPS) * ngain[...]).astype(BF16)
    nrm[...] = normed
    loads["w_up"].wait()
    pre = dot(normed, w_up[...])
    tanh = jnp.tanh(GC * (pre + GA * pre * pre * pre))
    hidden = (0.5 * pre * (1.0 + tanh)).astype(BF16)
    gd[...] = 0.5 * (1.0 + tanh) + 0.5 * pre * (1.0 - tanh * tanh) * (GC * (1.0 + 3.0 * GA * pre * pre))
    loads["w_proj"].wait()
    loads["w_down"].wait()
    wfull[y, x, core] = w_proj[...]
    for j in range(2):
        cs[j] = dot(hidden, w_down[:, at((1 - core) * 2 + j, 512)]).astype(BF16)
    h_all[z] = hidden.T
    me.met()
    to_core = [send(cs.at[j], cr.at[j], me.other_core()) for j in range(2)]
    w_y = [send(w_proj, wfull.at[y, x, core], me.along_y(i)) for i in (1, 2, 3)]
    to_x = []
    for j in range(2):
        own = dot(hidden, w_down[:, at(core * 2 + j, 512)])
        to_core[j].wait_recv()
        xs[j] = (own + cr[j].astype(F32)).astype(BF16).reshape(4, 4, 16, 512)
        to_x.append(
            [send(xs.at[j, :, lax.rem(x + i, 4)], xr.at[j, i - 1], me.along_x(i)) for i in (2, 1, 3)]
        )
    h_to = [send(h_all.at[z], h_all.at[z], me.along_z(i)) for i in (4, 3, 5, 2, 6, 1, 7)]
    for name in ("plen", "fgain", "quer", "assign", "valid"):
        loads[name].wait()
    vcol[...] = jnp.broadcast_to(valid[...].astype(F32), (128, 256)).T
    for copy in w_y:
        copy.wait_recv()
    to_y = []
    for j in range(2):
        for copy in to_x[j]:
            copy.wait_recv()
        total = xs[j, :, x].astype(F32)
        for i in range(3):
            total += xr[j, i].astype(F32)
        ys[j] = total.astype(BF16)
        to_y.append([send(ys.at[j, lax.rem(y + i, 4)], yr.at[j, i - 1], me.along_y(i)) for i in (2, 1, 3)])
    w_x = [send(wfull.at[:, x, core], wfull.at[:, x, core], me.along_x(i)) for i in (1, 2, 3)]
    for j in range(2):
        for copy in to_y[j]:
            copy.wait_recv()
        total = ys[j, y].astype(F32)
        for i in range(3):
            total += yr[j, i].astype(F32)
        lo[core, :, j * 512 : (j + 1) * 512] = total
    half = send(lo.at[core], lo.at[core], me.other_core())
    for copy in w_x:
        copy.wait_recv()
    w_core = send(wfull.at[:, :, core], wfull.at[:, :, core], me.other_core())
    half.wait_recv()
    layer_out = tok[at(chip, 16), :].astype(F32) + jnp.concatenate([lo[0], lo[1]], axis=1)
    centred = layer_out - jnp.mean(layer_out, axis=1, keepdims=True)
    inv_scale = lax.rsqrt(jnp.mean(centred * centred, axis=1, keepdims=True) + EPS)
    out_hat = centred * inv_scale
    final = out_hat * fgain[...]
    pool_weight = pool_weights(plen, chip)
    pooled = jnp.sum(final * pool_weight, axis=0, keepdims=True)
    pooled_low = pooled.astype(BF16)
    w_core.wait_recv()
    feat = dot(jnp.broadcast_to(pooled_low, (16, 2048)), wfull[...].reshape(2048, 256))
    frow[chip] = feat[:1].astype(BF16).astype(F32)
    to_plane = [send(frow.at[chip], frow.at[chip], me.in_plane(i)) for i in range(1, 16)]
    rounded = pooled_low.astype(F32)
    for k in range(16):
        psend[k] = rounded[:, k * 128 : (k + 1) * 128]
    prow[chip] = psend[chip]
    pooled_to = [send(psend.at[lax.rem(chip + i, 16)], prow.at[chip], me.in_plane(i)) for i in range(1, 16)]
    n_t[...] = nrm[...].T
    for copy in to_plane:
        copy.wait_recv()
    allf[t] = jnp.concatenate([frow[k] for k in range(16)], axis=0).astype(BF16)
    to_text = [send(allf.at[t], allf.at[t], me.in_text(i)) for i in range(1, 16)]
    for copy in pooled_to:
        copy.wait_recv()
    pj[t, :, 256:] = jnp.concatenate([prow[k] for k in range(16)], axis=0).astype(BF16)
    for copy in to_text:
        copy.wait_recv()

    features = allf[...].reshape(256, 256)
    score[...] = dot(features, quer[...], ((1,), (1,)))
    chosen = assign[...]

    @pl.loop(0, 16)
    def _(r):
        spot = at(r, 16)
        s = score[spot, :] * SCORE_SCALE + LOGIT_BIAS
        concept = lax.broadcasted_iota(jnp.int32, (16, 1100), 0) + r * 16
        hit = concept == chosen
        u = jnp.where(hit, -s, s)
        e = jnp.exp(-jnp.abs(u))
        more = 1.0 / (1.0 + e)
        less = e * more
        p = jnp.where(u >= 0.0, more, less)
        q = jnp.where(u >= 0.0, less, more)
        soft = jnp.maximum(u, 0.0) + jnp.log1p(e)
        factor = jnp.where(hit, -ALPHA, 1.0 - ALPHA) * vcol[spot, :1]
        sgrad[spot, :] = (factor * p * p * (p + 2.0 * q * soft)).astype(BF16)

    terms = dot(sgrad[...], quer[...]) * (SCORE_SCALE / IMAGES)
    halves = (terms[:, :128], terms[:, 128:])
    mine = jnp.where(core == 0, halves[0], halves[1])
    fcs[...] = jnp.where(core == 0, halves[1], halves[0]).astype(BF16)
    to_core = send(fcs, fcr, me.other_core())
    to_core.wait_recv()
    ts[...] = (mine + fcr[...].astype(F32)).astype(BF16).reshape(16, 16, 128)
    to_text2 = [send(ts.at[lax.rem(t + i, 16)], tr.at[i - 1], me.in_text(i)) for i in range(1, 16)]
    query_grad = dot(sgrad[...], features, ((0,), (0,))) * SCORE_SCALE
    qg[pl.ds(0, 1100, stride=2), :] = query_grad[:, :128]
    qg[pl.ds(1, 1100, stride=2), :] = query_grad[:, 128:]
    store(qg, qg_h)
    total = ts[t].astype(F32)
    for i in range(15):
        to_text2[i].wait_recv()
        total += tr[i].astype(F32)
    for k in range(16):
        rsend[k] = total[k : k + 1]
    rgot[core, chip] = rsend[chip]
    to_rows = [send(rsend.at[chip], rgot.at[core, chip], me.other_core())]
    for i in range(1, 16):
        there = rsend.at[lax.rem(chip + i, 16)]
        to_rows.append(send(there, rgot.at[core, chip], me.in_plane(i)))
        to_rows.append(send(there, rgot.at[core, chip], me.in_plane(i, 1)))
    for copy in to_rows:
        copy.wait_recv()
    sums = []
    for c in range(2):
        total = rgot[c, 0]
        for k in range(1, 16):
            total += rgot[c, k]
        sums.append(total)
    row = jnp.concatenate(sums, axis=1)
    grow[chip] = row
    high = row.astype(BF16).astype(F32)
    middle = (row - high).astype(BF16).astype(F32)
    low = row - high - middle
    part = lax.broadcasted_iota(jnp.int32, (16, 256), 0)
    rows = jnp.where(part == 0, high, jnp.where(part == 1, middle, jnp.where(part == 2, low, 0.0)))
    pooled_grad = jnp.sum(
        dot(rows.astype(BF16), wfull[...].reshape(2048, 256), ((1,), (1,))), axis=0, keepdims=True
    )
    hat = pooled_grad * fgain[...]
    first = jnp.mean(hat, axis=1, keepdims=True)
    second = jnp.mean(hat * out_hat, axis=1, keepdims=True)
    out_grad = ((hat - first - out_hat * second) * (pool_weight * inv_scale)).astype(BF16)
    og[0, y, x] = out_grad[:, :1024]
    og[1, y, x] = out_grad[:, 1024:]
    own = og.at[core, y, x]
    to_y = [send(own, own, me.along_y(i)) for i in (2, 1, 3)]
    waves = [[send(own, own, me.along_x(i)) for i in (2, 1, 3)]]
    for k in range(16):
        ogz[k] = out_grad[:, 128 * k : 128 * k + 128]
    dg[core, y, x, z] = ogz[2 * z + core]
    z_to = [
        send(ogz.at[lax.rem(z + i, 8) * 2 + core], dg.at[core, y, x, z], me.along_z(i))
        for i in (4, 3, 5, 2, 6, 1, 7)
    ]
    to_grow = [send(grow.at[chip], grow.at[chip], me.in_plane(i)) for i in range(1, 16)]

    def spread_y(to_y, buf, waves, to_other):
        for copy, i in ((to_y[1], 1), (to_y[2], 3), (to_y[0], 2)):
            copy.wait_recv()
            block = buf.at[core, lax.rem(y + 4 - i, 4), x]
            waves.append([send(block, block, me.along_x(j)) for j in (2, 1, 3)])
            to_other.append(send(block, block, me.other_core()))

    def spread_x(buf, waves, to_other):
        for wave, i in zip(waves, (0, 1, 3, 2)):
            for copy, j in zip(wave, (2, 1, 3)):
                copy.wait_recv()
                block = buf.at[core, lax.rem(y + 4 - i, 4), lax.rem(x + 4 - j, 4)]
                to_other.append(send(block, block, me.other_core()))

    to_other = []
    spread_y(to_y, og, waves, to_other)
    for copy in z_to:
        copy.wait_recv()
    own = dg.at[core, y, x]
    dg_y = [send(own, own, me.along_y(i)) for i in (2, 1, 3)]
    dg_waves = [[send(own, own, me.along_x(i)) for i in (2, 1, 3)]]
    dg_other = [send(own, own, me.other_core())]
    for copy in to_grow:
        copy.wait_recv()
    pj[t, :, :256] = jnp.concatenate([grow[k] for k in range(16)], axis=0).astype(BF16)
    pj_to = [send(pj.at[t], pj.at[t], me.in_text(i)) for i in range(1, 16)]
    spread_x(og, waves, to_other)
    spread_y(dg_y, dg, dg_waves, dg_other)
    for copy in to_other:
        copy.wait_recv()
    halves = [og[h].reshape(256, 1024) for h in range(2)]
    hidden_grad = dot(halves[0], w_down[:, :1024], ((1,), (1,))) + dot(halves[1], w_down[:, 1024:], ((1,), (1,)))
    pre_grad = (hidden_grad * gd[...]).astype(BF16)
    us[...] = dot(n_t[...], pre_grad).astype(BF16).reshape(8, 2, 128, 256)
    order = (4, 3, 5, 2, 6, 1, 7, 0)
    up_y, up_z = {}, {}
    for i in order:
        up_y[i] = send(us.at[lax.rem(z + i, 8), 1 - yl], uyr.at[i], me.across())

    def onward(i):
        up_y[i].wait_recv()
        uz[i - 1] = (us[lax.rem(z + i, 8), yl].astype(F32) + uyr[i].astype(F32)).astype(BF16)
        up_z[i] = send(uz.at[i - 1], ur.at[i - 1], me.along_z(i))

    for i in order[:4]:
        onward(i)
    spread_x(dg, dg_waves, dg_other)
    for i in order[4:6]:
        onward(i)
    for copy in dg_other + h_to:
        copy.wait_recv()

    def down_product(h):
        total = dot(h_all[0], dg[h, :, :, 0].reshape(256, 128))
        for k in range(1, 8):
            total += dot(h_all[k], dg[h, :, :, k].reshape(256, 128))
        return total

    dp[...] = down_product(1 - yl).astype(BF16)
    dp_to = send(dp, dpr, me.across())
    onward(order[6])
    down_own = down_product(yl)
    for copy in pj_to:
        copy.wait_recv()
    pjf[...] = dot(pj[:, :, 256:].reshape(256, 128), pj[:, :, :256].reshape(256, 256), ((0,), (0,)))
    proj_o[...] = pjf[at(core, 64), :]
    store(proj_o, proj_h)
    dp_to.wait_recv()
    down_o[...] = down_own + dpr[...].astype(F32)
    store(down_o, down_h)
    up_y[0].wait_recv()
    total = us[z, yl].astype(F32) + uyr[0].astype(F32)
    for i in (4, 3, 5, 2, 6, 1, 7):
        up_z[i].wait_recv()
        total += ur[i - 1].astype(F32)
    up_o[...] = total
    store(up_o, up_h)
    send.drain()
    for copy in stores:
        copy.wait()


def hand_out_kernel(a, b, c, d, a_o, b_o, c_o, d_o, a_v, b_v, c_v, d_v, sems):
    parts = []
    for lo, n in ((0, 552), (552, 552), (1104, 552), (1656, 544)):
        rows = pl.ds(lo, n)
        parts.append((d.at[rows], d_v.at[rows], d_o.at[rows]))
    parts += [(a, a_v, a_o), (b, b_v, b_o), (c, c_v, c_o)]
    loads = [pltpu.make_async_copy(src, mid, sems.at[0, n]) for n, (src, mid, _) in enumerate(parts)]
    stores = [pltpu.make_async_copy(mid, dst, sems.at[1, n]) for n, (_, mid, dst) in enumerate(parts)]
    for load in loads:
        load.start()
    for load, store in zip(loads, stores):
        load.wait()
        store.start()
    for store in stores:
        store.wait()


def hand_out(arrays):
    return pl.pallas_call(
        hand_out_kernel,
        name="hand_out",
        in_specs=[pl.BlockSpec(memory_space=pltpu.HBM)] * 4,
        out_specs=[pl.BlockSpec(memory_space=pltpu.HBM)] * 4,
        out_shape=[jax.ShapeDtypeStruct(a.shape, a.dtype) for a in arrays],
        scratch_shapes=[pltpu.VMEM(a.shape, a.dtype) for a in arrays] + [pltpu.SemaphoreType.DMA((2, 7))],
        compiler_params=pltpu.CompilerParams(vmem_limit_bytes=62 << 20),
    )(*arrays)


def step(*args):
    return pl.pallas_call(
        step_kernel,
        name="step",
        in_specs=[pl.BlockSpec(memory_space=pltpu.HBM)] * 10,
        out_specs=[pl.BlockSpec(memory_space=pltpu.HBM)] * 4,
        out_shape=(
            jax.ShapeDtypeStruct((128, 256), F32),
            jax.ShapeDtypeStruct((256, 128), F32),
            jax.ShapeDtypeStruct((64, 256), F32),
            jax.ShapeDtypeStruct((2200, 128), F32),
        ),
        scratch_shapes=[
            pltpu.VMEM((1, 16), jnp.int32),
            pltpu.VMEM((256, 2048), BF16),
            pltpu.VMEM((1, 2048), F32),
            pltpu.VMEM((2048, 256), BF16),
            pltpu.VMEM((256, 2048), BF16),
            pltpu.VMEM((1, 2048), F32),
            pltpu.VMEM((64, 256), BF16),
            pltpu.VMEM((1100, 256), BF16),
            pltpu.VMEM((1, 1100), jnp.int32),
            pltpu.VMEM((1, 256), jnp.int32),
            pltpu.VMEM((256, 2048), BF16),
            pltpu.VMEM((256, 256), F32),
            pltpu.VMEM((2, 256, 512), BF16),
            pltpu.VMEM((2, 256, 512), BF16),
            pltpu.VMEM((2, 4, 4, 16, 512), BF16),
            pltpu.VMEM((2, 3, 4, 16, 512), BF16),
            pltpu.VMEM((2, 4, 16, 512), BF16),
            pltpu.VMEM((2, 3, 16, 512), BF16),
            pltpu.VMEM((2, 16, 1024), F32),
            pltpu.VMEM((4, 4, 2, 64, 256), BF16),
            pltpu.VMEM((16, 1, 256), F32),
            pltpu.VMEM((16, 1, 128), F32),
            pltpu.VMEM((16, 1, 128), F32),
            pltpu.VMEM((16, 16, 256), BF16),
            pltpu.VMEM((256, 128), F32),
            pltpu.VMEM((256, 1100), F32),
            pltpu.VMEM((256, 1100), BF16),
            pltpu.VMEM((2200, 128), F32),
            pltpu.VMEM((128, 256), F32),
            pltpu.VMEM((256, 128), F32),
            pltpu.VMEM((64, 256), F32),
            pltpu.VMEM((256, 128), BF16),
            pltpu.VMEM((256, 128), BF16),
            pltpu.VMEM((16, 16, 128), BF16),
            pltpu.VMEM((15, 16, 128), BF16),
            pltpu.VMEM((16, 1, 128), F32),
            pltpu.VMEM((2, 16, 1, 128), F32),
            pltpu.VMEM((16, 1, 256), F32),
            pltpu.VMEM((16, 16, 384), BF16),
            pltpu.VMEM((128, 256), F32),
            pltpu.VMEM((2, 4, 4, 16, 1024), BF16),
            pltpu.VMEM((8, 256, 256), BF16),
            pltpu.VMEM((2048, 256), BF16),
            pltpu.VMEM((16, 16, 128), BF16),
            pltpu.VMEM((2, 4, 4, 8, 16, 128), BF16),
            pltpu.VMEM((256, 128), BF16),
            pltpu.VMEM((256, 128), BF16),
            pltpu.VMEM((8, 2, 128, 256), BF16),
            pltpu.VMEM((8, 128, 256), BF16),
            pltpu.VMEM((7, 128, 256), BF16),
            pltpu.VMEM((7, 128, 256), BF16),
            pltpu.SemaphoreType.DMA((10,)),
            pltpu.SemaphoreType.DMA((4,)),
            pltpu.SemaphoreType.DMA((COPIES,)),
            pltpu.SemaphoreType.DMA((COPIES,)),
        ],
        compiler_params=pltpu.CompilerParams(
            collective_id=0, has_side_effects=True, vmem_limit_bytes=62 << 20
        ),
    )(*args)


def body(
    prompt_embeds, prompt_len, norm_gain, w_up, w_down, final_gain, w_proj, queries, assign, valid
):
    results = step(
        prompt_len.reshape(1, 16),
        prompt_embeds.reshape(256, 2048),
        norm_gain.reshape(1, 2048),
        w_up,
        w_down,
        final_gain.reshape(1, 2048),
        w_proj,
        queries.reshape(1100, 256),
        assign,
        valid,
    )
    up_grad, down_grad, proj_grad, query_grad = hand_out(results)
    return (up_grad, down_grad, proj_grad, query_grad.reshape(1, 1100, 256))


def solution(mesh):
    return jax.shard_map(
        body,
        mesh=mesh,
        in_specs=(
            P("text", None, None),
            P("text"),
            P(),
            P(None, "det"),
            P("det", None),
            P(),
            P("det", None),
            P(("text", "det"), None, None),
            P(("text", "det"), None),
            P(("text", "det"), None),
        ),
        out_specs=(
            P("text", "det"),
            P("det", "text"),
            P("det", None),
            P(("text", "det"), None, None),
        ),
        check_vma=False,
    )
```

```python
import jax
import jax.numpy as jnp
from jax import lax
from jax.experimental import pallas as pl
from jax.experimental.pallas import tpu as pltpu
from jax.sharding import PartitionSpec as P

EPS = 1e-05
ALPHA = 0.25
LOGIT_BIAS = -2.0
F32 = jnp.float32
BF16 = jnp.bfloat16
MESH = pl.DeviceIdType.MESH
GC = 0.7978845608028654
GA = 0.044715


class Place:
    def __init__(self):
        self.t = lax.axis_index("text")
        self.d = lax.axis_index("det")
        self.core = lax.rem(self.d, 2)
        self.chip = self.d // 2
        self.x = lax.rem(self.chip, 4)
        self.y = self.chip // 4
        self.z = self.t // 2
        self.yl = lax.rem(self.t, 2)

    def other_core(self):
        return {"det": self.d + 1 - 2 * self.core}

    def along_x(self, i):
        return {"det": (self.y * 4 + lax.rem(self.x + i, 4)) * 2 + self.core}

    def along_y(self, i):
        return {"det": (lax.rem(self.y + i, 4) * 4 + self.x) * 2 + self.core}

    def in_plane(self, i):
        return {"det": lax.rem(self.chip + i, 16) * 2 + self.core}

    def in_text(self, i):
        return {"text": lax.rem(self.t + i, 16)}

    def along_z(self, i):
        return {"text": lax.rem(self.z + i, 8) * 2 + self.yl}

    def across(self):
        return {"text": self.t + 1 - 2 * self.yl}

    def greet(self):
        barrier = pltpu.get_barrier_semaphore()
        pl.semaphore_signal(barrier, inc=1, device_id=self.other_core(), device_id_type=MESH)
        for i in range(1, 16):
            pl.semaphore_signal(barrier, inc=1, device_id=self.in_plane(i), device_id_type=MESH)
            pl.semaphore_signal(barrier, inc=1, device_id=self.in_text(i), device_id_type=MESH)

    def met(self):
        pl.semaphore_wait(pltpu.get_barrier_semaphore(), 31)


class Sends:
    def __init__(self, send_sems, recv_sems):
        self.send_sems, self.recv_sems, self.used = send_sems, recv_sems, 0
        self.flying = []

    def __call__(self, src, dst, to):
        copy = pltpu.make_async_remote_copy(
            src_ref=src,
            dst_ref=dst,
            send_sem=self.send_sems.at[self.used],
            recv_sem=self.recv_sems.at[self.used],
            device_id=to,
            device_id_type=MESH,
        )
        self.used += 1
        copy.start()
        self.flying.append(copy)
        return copy

    def drain(self):
        for copy in self.flying:
            copy.wait_send()


def at(i, n):
    return pl.ds(pl.multiple_of(i * n, n), n)


def dot(a, b, dims=((1,), (0,))):
    return lax.dot_general(a, b, (dims, ((), ())), preferred_element_type=F32)


def pool_weights(plen, chip):
    lane = lax.broadcasted_iota(jnp.int32, (16, 16), 1)
    length = jnp.sum(jnp.where(lane == chip, plen[...], 0).astype(F32), axis=1, keepdims=True)
    slot = lax.broadcasted_iota(jnp.int32, (16, 1), 0).astype(F32)
    return jnp.where(slot < length, 1.0 / length, 0.0)


COPIES = sum(
    (2, 3, 6, 7, 3, 6, 1, 1, 15, 3, 12, 15, 7, 15, 15, 3, 12, 16, 1, 15, 15, 1, 15, 7, 8, 7, 1)
)
SCORE_SCALE = 256 ** (-0.5)
IMAGES = 512


def step_kernel(
    plen_h, tok_h, ngain_h, w_up_h, w_down_h, fgain_h, w_proj_h, quer_h, assign_h, valid_h,
    up_h, down_h, proj_h, qg_h,
    plen, tok, ngain, w_up, w_down, fgain, w_proj, quer, assign, valid,
    nrm, gd, cs, cr, xs, xr, ys, yr, lo, wfull, frow, psend, prow, allf, vcol, score, sgrad, qg, up_o, down_o, proj_o,
    fcs, fcr, ts, tr, ps, pr, fgb, gs, cols, scg, gz, pj, pjf, oh, og, h_all, n_t, ohz, dg, dp, dpr,
    us, uyr, uz, ur, load_sems, store_sems, send_sems, recv_sems,
):
    me = Place()
    send = Sends(send_sems, recv_sems)
    core, chip, x, y, t, z, yl = me.core, me.chip, me.x, me.y, me.t, me.z, me.yl
    me.greet()
    loads = {}
    for n, (name, src, dst) in enumerate((
        ("tok", tok_h, tok), ("ngain", ngain_h, ngain), ("w_up", w_up_h, w_up), ("w_down", w_down_h, w_down),
        ("w_proj", w_proj_h, w_proj), ("plen", plen_h, plen), ("fgain", fgain_h, fgain),
        ("quer", quer_h, quer), ("assign", assign_h, assign), ("valid", valid_h, valid),
    )):
        loads[name] = pltpu.make_async_copy(src, dst, load_sems.at[n])
        loads[name].start()
    stores = []

    def store(src, dst):
        copy = pltpu.make_async_copy(src, dst, store_sems.at[len(stores)])
        copy.start()
        stores.append(copy)

    loads["tok"].wait()
    loads["ngain"].wait()
    tokens = tok[...].astype(F32)
    centred = tokens - jnp.mean(tokens, axis=1, keepdims=True)
    variance = jnp.mean(centred * centred, axis=1, keepdims=True)
    normed = (centred * lax.rsqrt(variance + EPS) * ngain[...]).astype(BF16)
    nrm[...] = normed
    loads["w_up"].wait()
    pre = dot(normed, w_up[...])
    tanh = jnp.tanh(GC * (pre + GA * pre * pre * pre))
    hidden = (0.5 * pre * (1.0 + tanh)).astype(BF16)
    gd[...] = 0.5 * (1.0 + tanh) + 0.5 * pre * (1.0 - tanh * tanh) * (GC * (1.0 + 3.0 * GA * pre * pre))
    loads["w_proj"].wait()
    loads["w_down"].wait()
    wfull[y, x, core] = w_proj[...]
    for j in range(2):
        cs[j] = dot(hidden, w_down[:, at((1 - core) * 2 + j, 512)]).astype(BF16)
    h_all[z] = hidden.T
    me.met()
    to_core = [send(cs.at[j], cr.at[j], me.other_core()) for j in range(2)]
    w_y = [send(w_proj, wfull.at[y, x, core], me.along_y(i)) for i in (1, 2, 3)]
    to_x = []
    for j in range(2):
        own = dot(hidden, w_down[:, at(core * 2 + j, 512)])
        to_core[j].wait_recv()
        xs[j] = (own + cr[j].astype(F32)).astype(BF16).reshape(4, 4, 16, 512)
        to_x.append(
            [send(xs.at[j, :, lax.rem(x + i, 4)], xr.at[j, i - 1], me.along_x(i)) for i in (2, 1, 3)]
        )
    h_to = [send(h_all.at[z], h_all.at[z], me.along_z(i)) for i in (4, 3, 5, 2, 6, 1, 7)]
    for name in ("plen", "fgain", "quer", "assign", "valid"):
        loads[name].wait()
    vcol[...] = jnp.broadcast_to(valid[...].astype(F32), (128, 256)).T
    for copy in w_y:
        copy.wait_recv()
    w_x = [send(wfull.at[:, x, core], wfull.at[:, x, core], me.along_x(i)) for i in (1, 2, 3)]
    to_y = []
    for j in range(2):
        for copy in to_x[j]:
            copy.wait_recv()
        total = xs[j, :, x].astype(F32)
        for i in range(3):
            total += xr[j, i].astype(F32)
        ys[j] = total.astype(BF16)
        to_y.append([send(ys.at[j, lax.rem(y + i, 4)], yr.at[j, i - 1], me.along_y(i)) for i in (2, 1, 3)])
    for copy in w_x:
        copy.wait_recv()
    w_core = send(wfull.at[:, :, core], wfull.at[:, :, core], me.other_core())
    for j in range(2):
        for copy in to_y[j]:
            copy.wait_recv()
        total = ys[j, y].astype(F32)
        for i in range(3):
            total += yr[j, i].astype(F32)
        lo[core, :, j * 512 : (j + 1) * 512] = total
    half = send(lo.at[core], lo.at[core], me.other_core())
    half.wait_recv()
    layer_out = tok[at(chip, 16), :].astype(F32) + jnp.concatenate([lo[0], lo[1]], axis=1)
    centred = layer_out - jnp.mean(layer_out, axis=1, keepdims=True)
    inv_scale = lax.rsqrt(jnp.mean(centred * centred, axis=1, keepdims=True) + EPS)
    out_hat = centred * inv_scale
    final = out_hat * fgain[...]
    pool_weight = pool_weights(plen, chip)
    pooled = jnp.sum(final * pool_weight, axis=0, keepdims=True)
    pooled_low = pooled.astype(BF16)
    w_core.wait_recv()
    feat = dot(jnp.broadcast_to(pooled_low, (16, 2048)), wfull[...].reshape(2048, 256))
    frow[chip] = feat[:1].astype(BF16).astype(F32)
    to_plane = [send(frow.at[chip], frow.at[chip], me.in_plane(i)) for i in range(1, 16)]
    hat_low = out_hat.astype(BF16)
    oh[0, chip] = hat_low[:, :1024]
    oh[1, chip] = hat_low[:, 1024:]
    own = oh.at[core, chip]
    oh_y = [send(own, own, me.along_y(i)) for i in (2, 1, 3)]
    oh_waves = [[send(own, own, me.along_x(i)) for i in (2, 1, 3)]]
    for k in range(16):
        ohz[k] = hat_low[:, 128 * k : 128 * k + 128]
    dg[core, chip, z] = ohz[2 * z + core]
    z_to = [
        send(ohz.at[lax.rem(z + i, 8) * 2 + core], dg.at[core, chip, z], me.along_z(i))
        for i in (4, 3, 5, 2, 6, 1, 7)
    ]
    rounded = pooled_low.astype(F32)
    diagonal = lax.broadcasted_iota(jnp.int32, (16, 128), 0) == lax.broadcasted_iota(jnp.int32, (16, 128), 1)
    scale_row = jnp.sum(jnp.where(diagonal, pool_weight * inv_scale, 0.0), axis=0, keepdims=True)
    for k in range(16):
        psend[k] = jnp.concatenate([rounded[:, k * 128 : (k + 1) * 128], scale_row], axis=1)
    prow[chip] = psend[chip]
    pooled_to = [send(psend.at[lax.rem(chip + i, 16)], prow.at[chip], me.in_plane(i)) for i in range(1, 16)]
    n_t[...] = nrm[...].T
    for copy in to_plane:
        copy.wait_recv()
    allf[t] = jnp.concatenate([frow[k] for k in range(16)], axis=0).astype(BF16)
    to_text = [send(allf.at[t], allf.at[t], me.in_text(i)) for i in range(1, 16)]

    def spread_y(to_y, buf, waves, to_other):
        for copy, i in ((to_y[1], 1), (to_y[2], 3), (to_y[0], 2)):
            copy.wait_recv()
            block = buf.at[core, lax.rem(y + 4 - i, 4) * 4 + x]
            waves.append([send(block, block, me.along_x(j)) for j in (2, 1, 3)])
            to_other.append(send(block, block, me.other_core()))

    def spread_x(buf, waves, to_other):
        for wave, i in zip(waves, (0, 1, 3, 2)):
            for copy, j in zip(wave, (2, 1, 3)):
                copy.wait_recv()
                block = buf.at[core, lax.rem(y + 4 - i, 4) * 4 + lax.rem(x + 4 - j, 4)]
                to_other.append(send(block, block, me.other_core()))

    oh_other = []
    spread_y(oh_y, oh, oh_waves, oh_other)
    for copy in pooled_to:
        copy.wait_recv()
    pj[t, :, 256:] = jnp.concatenate([prow[k] for k in range(16)], axis=0)[:, :128].astype(BF16)
    for copy in z_to:
        copy.wait_recv()
    own = dg.at[core, chip]
    dg_y = [send(own, own, me.along_y(i)) for i in (2, 1, 3)]
    dg_waves = [[send(own, own, me.along_x(i)) for i in (2, 1, 3)]]
    dg_other = [send(own, own, me.other_core())]
    for copy in to_text:
        copy.wait_recv()

    features = allf[...].reshape(256, 256)
    score[...] = dot(features, quer[...], ((1,), (1,)))
    chosen = assign[...]

    @pl.loop(0, 16)
    def _(r):
        spot = at(r, 16)
        s = score[spot, :] * SCORE_SCALE + LOGIT_BIAS
        concept = lax.broadcasted_iota(jnp.int32, (16, 1100), 0) + r * 16
        hit = concept == chosen
        u = jnp.where(hit, -s, s)
        e = jnp.exp(-jnp.abs(u))
        more = 1.0 / (1.0 + e)
        less = e * more
        p = jnp.where(u >= 0.0, more, less)
        q = jnp.where(u >= 0.0, less, more)
        soft = jnp.maximum(u, 0.0) + jnp.log1p(e)
        factor = jnp.where(hit, -ALPHA, 1.0 - ALPHA) * vcol[spot, :1]
        sgrad[spot, :] = (factor * p * p * (p + 2.0 * q * soft)).astype(BF16)

    terms = dot(sgrad[...], quer[...]) * (SCORE_SCALE / IMAGES)
    halves = (terms[:, :128], terms[:, 128:])
    mine = jnp.where(core == 0, halves[0], halves[1])
    fcs[...] = jnp.where(core == 0, halves[1], halves[0]).astype(BF16)
    to_core = send(fcs, fcr, me.other_core())
    spread_y(dg_y, dg, dg_waves, dg_other)
    to_core.wait_recv()
    ts[...] = (mine + fcr[...].astype(F32)).astype(BF16).reshape(16, 16, 128)
    to_text2 = [send(ts.at[lax.rem(t + i, 16)], tr.at[i - 1], me.in_text(i)) for i in range(1, 16)]
    query_grad = dot(sgrad[...], features, ((0,), (0,))) * SCORE_SCALE
    qg[pl.ds(0, 1100, stride=2), :] = query_grad[:, :128]
    qg[pl.ds(1, 1100, stride=2), :] = query_grad[:, 128:]
    store(qg, qg_h)
    spread_x(oh, oh_waves, oh_other)
    for copy in oh_other:
        copy.wait_recv()
    total = ts[t].astype(F32)
    for i in range(15):
        to_text2[i].wait_recv()
        total += tr[i].astype(F32)
    ps[...] = total.astype(BF16)
    to_plane2 = [send(ps, pr.at[i - 1], me.in_plane(i)) for i in range(1, 16)]
    spread_x(dg, dg_waves, dg_other)
    for i in range(15):
        to_plane2[i].wait_recv()
        total += pr[i].astype(F32)
    fgb[core] = total
    half = send(fgb.at[core], fgb.at[core], me.other_core())
    half.wait_recv()
    feat_grad = jnp.concatenate([fgb[0], fgb[1]], axis=1)
    pj[t, :, :256] = feat_grad.astype(BF16)
    pj_to = [send(pj.at[t], pj.at[t], me.in_text(i)) for i in range(1, 16)]
    high = feat_grad.astype(BF16)
    middle = (feat_grad - high.astype(F32)).astype(BF16)
    low = (feat_grad - high.astype(F32) - middle.astype(F32)).astype(BF16)
    parts = dot(jnp.concatenate([high, middle, low], axis=0), wfull[...].reshape(2048, 256), ((1,), (1,)))
    gs[...] = (parts[:16] + parts[16:32] + parts[32:]) * fgain[...]
    lane = lax.broadcasted_iota(jnp.int32, (16, 128), 1)
    for k in range(16):
        hat = gs[k : k + 1, :]
        out_hat = jnp.concatenate([oh[0, k], oh[1, k]], axis=1).astype(F32)
        first = jnp.mean(hat, axis=1, keepdims=True)
        second = jnp.mean(hat * out_hat, axis=1, keepdims=True)
        scale = jnp.sum(jnp.where(diagonal, prow[k][:, 128:], 0.0), axis=1, keepdims=True)
        og[16 * k : 16 * k + 16, :] = ((hat - first - out_hat * second) * scale).astype(BF16)
        cols[16 * k : 16 * k + 16, :] = jnp.where(
            lane == 0, scale, jnp.where(lane == 1, first, jnp.where(lane == 2, second, 0.0))
        )
    scg[z] = cols[...].T[:8]
    sc_to = [send(scg.at[z], scg.at[z], me.along_z(i)) for i in (4, 3, 5, 2, 6, 1, 7)]
    hidden_grad = dot(og[...], w_down[...], ((1,), (1,)))
    pre_grad = (hidden_grad * gd[...]).astype(BF16)
    us[...] = dot(n_t[...], pre_grad).astype(BF16).reshape(8, 2, 128, 256)
    order = (4, 3, 5, 2, 6, 1, 7, 0)
    up_y, up_z = {}, {}
    for i in order:
        up_y[i] = send(us.at[lax.rem(z + i, 8), 1 - yl], uyr.at[i], me.across())

    def onward(i):
        up_y[i].wait_recv()
        uz[i - 1] = (us[lax.rem(z + i, 8), yl].astype(F32) + uyr[i].astype(F32)).astype(BF16)
        up_z[i] = send(uz.at[i - 1], ur.at[i - 1], me.along_z(i))

    for i in order[:4]:
        onward(i)
    for copy in dg_other + h_to + sc_to + pj_to:
        copy.wait_recv()
    fg_group = jnp.concatenate([pj[2 * k + yl, :, :256] for k in range(8)], axis=0)
    w_group = wfull[z // 2, pl.ds(2 * lax.rem(z, 2), 2)].reshape(256, 256)
    gz[...] = dot(fg_group, w_group, ((1,), (1,))) * fgain[:, at(z, 256)]
    product = jnp.zeros((256, 256), F32)
    for k in range(8):
        turned = jnp.concatenate([scg[k], jnp.zeros((120, 256), F32)], axis=0).T
        scale, first, second = turned[:, :1], turned[:, 1:2], turned[:, 2:3]
        hat = jnp.broadcast_to(gz[16 * k : 16 * k + 16][:, None, :], (16, 16, 256)).reshape(256, 256)
        out_hat = jnp.concatenate([dg[h, :, k].reshape(256, 128) for h in range(2)], axis=1).astype(F32)
        grads = ((hat - first - out_hat * second) * scale).astype(BF16)
        product += dot(h_all[k], grads)
    lower, upper = product[:, :128], product[:, 128:]
    dp[...] = jnp.where(yl == 0, upper, lower).astype(BF16)
    down_own = jnp.where(yl == 0, lower, upper)
    dp_to = send(dp, dpr, me.across())
    for i in order[4:6]:
        onward(i)
    onward(order[6])
    pjf[...] = dot(pj[:, :, 256:].reshape(256, 128), pj[:, :, :256].reshape(256, 256), ((0,), (0,)))
    proj_o[...] = pjf[at(core, 64), :]
    store(proj_o, proj_h)
    dp_to.wait_recv()
    down_o[...] = down_own + dpr[...].astype(F32)
    store(down_o, down_h)
    up_y[0].wait_recv()
    total = us[z, yl].astype(F32) + uyr[0].astype(F32)
    for i in (4, 3, 5, 2, 6, 1, 7):
        up_z[i].wait_recv()
        total += ur[i - 1].astype(F32)
    up_o[...] = total
    store(up_o, up_h)
    send.drain()
    for copy in stores:
        copy.wait()


def hand_out_kernel(a, b, c, d, a_o, b_o, c_o, d_o, a_v, b_v, c_v, d_v, sems):
    parts = []
    for lo, n in ((0, 552), (552, 552), (1104, 552), (1656, 544)):
        rows = pl.ds(lo, n)
        parts.append((d.at[rows], d_v.at[rows], d_o.at[rows]))
    parts += [(a, a_v, a_o), (b, b_v, b_o), (c, c_v, c_o)]
    loads = [pltpu.make_async_copy(src, mid, sems.at[0, n]) for n, (src, mid, _) in enumerate(parts)]
    stores = [pltpu.make_async_copy(mid, dst, sems.at[1, n]) for n, (_, mid, dst) in enumerate(parts)]
    for load in loads:
        load.start()
    for load, store in zip(loads, stores):
        load.wait()
        store.start()
    for store in stores:
        store.wait()


def hand_out(arrays):
    return pl.pallas_call(
        hand_out_kernel,
        name="hand_out",
        in_specs=[pl.BlockSpec(memory_space=pltpu.HBM)] * 4,
        out_specs=[pl.BlockSpec(memory_space=pltpu.HBM)] * 4,
        out_shape=[jax.ShapeDtypeStruct(a.shape, a.dtype) for a in arrays],
        scratch_shapes=[pltpu.VMEM(a.shape, a.dtype) for a in arrays] + [pltpu.SemaphoreType.DMA((2, 7))],
        compiler_params=pltpu.CompilerParams(vmem_limit_bytes=62 << 20),
    )(*arrays)


def step(*args):
    return pl.pallas_call(
        step_kernel,
        name="step",
        in_specs=[pl.BlockSpec(memory_space=pltpu.HBM)] * 10,
        out_specs=[pl.BlockSpec(memory_space=pltpu.HBM)] * 4,
        out_shape=(
            jax.ShapeDtypeStruct((128, 256), F32),
            jax.ShapeDtypeStruct((256, 128), F32),
            jax.ShapeDtypeStruct((64, 256), F32),
            jax.ShapeDtypeStruct((2200, 128), F32),
        ),
        scratch_shapes=[
            pltpu.VMEM((1, 16), jnp.int32),
            pltpu.VMEM((256, 2048), BF16),
            pltpu.VMEM((1, 2048), F32),
            pltpu.VMEM((2048, 256), BF16),
            pltpu.VMEM((256, 2048), BF16),
            pltpu.VMEM((1, 2048), F32),
            pltpu.VMEM((64, 256), BF16),
            pltpu.VMEM((1100, 256), BF16),
            pltpu.VMEM((1, 1100), jnp.int32),
            pltpu.VMEM((1, 256), jnp.int32),
            pltpu.VMEM((256, 2048), BF16),
            pltpu.VMEM((256, 256), F32),
            pltpu.VMEM((2, 256, 512), BF16),
            pltpu.VMEM((2, 256, 512), BF16),
            pltpu.VMEM((2, 4, 4, 16, 512), BF16),
            pltpu.VMEM((2, 3, 4, 16, 512), BF16),
            pltpu.VMEM((2, 4, 16, 512), BF16),
            pltpu.VMEM((2, 3, 16, 512), BF16),
            pltpu.VMEM((2, 16, 1024), F32),
            pltpu.VMEM((4, 4, 2, 64, 256), BF16),
            pltpu.VMEM((16, 1, 256), F32),
            pltpu.VMEM((16, 1, 256), F32),
            pltpu.VMEM((16, 1, 256), F32),
            pltpu.VMEM((16, 16, 256), BF16),
            pltpu.VMEM((256, 128), F32),
            pltpu.VMEM((256, 1100), F32),
            pltpu.VMEM((256, 1100), BF16),
            pltpu.VMEM((2200, 128), F32),
            pltpu.VMEM((128, 256), F32),
            pltpu.VMEM((256, 128), F32),
            pltpu.VMEM((64, 256), F32),
            pltpu.VMEM((256, 128), BF16),
            pltpu.VMEM((256, 128), BF16),
            pltpu.VMEM((16, 16, 128), BF16),
            pltpu.VMEM((15, 16, 128), BF16),
            pltpu.VMEM((16, 128), BF16),
            pltpu.VMEM((15, 16, 128), BF16),
            pltpu.VMEM((2, 16, 128), F32),
            pltpu.VMEM((16, 2048), F32),
            pltpu.VMEM((256, 128), F32),
            pltpu.VMEM((8, 8, 256), F32),
            pltpu.VMEM((128, 256), F32),
            pltpu.VMEM((16, 16, 384), BF16),
            pltpu.VMEM((128, 256), F32),
            pltpu.VMEM((2, 16, 16, 1024), BF16),
            pltpu.VMEM((256, 2048), BF16),
            pltpu.VMEM((8, 256, 256), BF16),
            pltpu.VMEM((2048, 256), BF16),
            pltpu.VMEM((16, 16, 128), BF16),
            pltpu.VMEM((2, 16, 8, 16, 128), BF16),
            pltpu.VMEM((256, 128), BF16),
            pltpu.VMEM((256, 128), BF16),
            pltpu.VMEM((8, 2, 128, 256), BF16),
            pltpu.VMEM((8, 128, 256), BF16),
            pltpu.VMEM((7, 128, 256), BF16),
            pltpu.VMEM((7, 128, 256), BF16),
            pltpu.SemaphoreType.DMA((10,)),
            pltpu.SemaphoreType.DMA((4,)),
            pltpu.SemaphoreType.DMA((COPIES,)),
            pltpu.SemaphoreType.DMA((COPIES,)),
        ],
        compiler_params=pltpu.CompilerParams(
            collective_id=0, has_side_effects=True, vmem_limit_bytes=62 << 20
        ),
    )(*args)


def body(
    prompt_embeds, prompt_len, norm_gain, w_up, w_down, final_gain, w_proj, queries, assign, valid
):
    results = step(
        prompt_len.reshape(1, 16),
        prompt_embeds.reshape(256, 2048),
        norm_gain.reshape(1, 2048),
        w_up,
        w_down,
        final_gain.reshape(1, 2048),
        w_proj,
        queries.reshape(1100, 256),
        assign,
        valid,
    )
    up_grad, down_grad, proj_grad, query_grad = hand_out(results)
    return (up_grad, down_grad, proj_grad, query_grad.reshape(1, 1100, 256))


def solution(mesh):
    return jax.shard_map(
        body,
        mesh=mesh,
        in_specs=(
            P("text", None, None),
            P("text"),
            P(),
            P(None, "det"),
            P("det", None),
            P(),
            P("det", None),
            P(("text", "det"), None, None),
            P(("text", "det"), None),
            P(("text", "det"), None),
        ),
        out_specs=(
            P("text", "det"),
            P("det", "text"),
            P("det", None),
            P(("text", "det"), None, None),
        ),
        check_vma=False,
    )
```

```python
import jax
import jax.numpy as jnp
from jax import lax
from jax.experimental import pallas as pl
from jax.experimental.pallas import tpu as pltpu
from jax.sharding import PartitionSpec as P

EPS = 1e-05
ALPHA = 0.25
LOGIT_BIAS = -2.0
F32 = jnp.float32
BF16 = jnp.bfloat16
MESH = pl.DeviceIdType.MESH
GC = 0.7978845608028654
GA = 0.044715


class Place:
    def __init__(self):
        self.t = lax.axis_index("text")
        self.d = lax.axis_index("det")
        self.core = lax.rem(self.d, 2)
        self.chip = self.d // 2
        self.x = lax.rem(self.chip, 4)
        self.y = self.chip // 4
        self.z = self.t // 2
        self.yl = lax.rem(self.t, 2)

    def other_core(self):
        return {"det": self.d + 1 - 2 * self.core}

    def along_x(self, i):
        return {"det": (self.y * 4 + lax.rem(self.x + i, 4)) * 2 + self.core}

    def along_y(self, i):
        return {"det": (lax.rem(self.y + i, 4) * 4 + self.x) * 2 + self.core}

    def in_plane(self, i):
        return {"det": lax.rem(self.chip + i, 16) * 2 + self.core}

    def in_text(self, i):
        return {"text": lax.rem(self.t + i, 16)}

    def along_z(self, i):
        return {"text": lax.rem(self.z + i, 8) * 2 + self.yl}

    def across(self):
        return {"text": self.t + 1 - 2 * self.yl}

    def greet(self):
        barrier = pltpu.get_barrier_semaphore()
        pl.semaphore_signal(barrier, inc=1, device_id=self.other_core(), device_id_type=MESH)
        for i in range(1, 16):
            pl.semaphore_signal(barrier, inc=1, device_id=self.in_plane(i), device_id_type=MESH)
            pl.semaphore_signal(barrier, inc=1, device_id=self.in_text(i), device_id_type=MESH)

    def met(self):
        pl.semaphore_wait(pltpu.get_barrier_semaphore(), 31)


class Sends:
    def __init__(self, send_sems, recv_sems):
        self.send_sems, self.recv_sems, self.used = send_sems, recv_sems, 0
        self.flying = []

    def __call__(self, src, dst, to):
        copy = pltpu.make_async_remote_copy(
            src_ref=src,
            dst_ref=dst,
            send_sem=self.send_sems.at[self.used],
            recv_sem=self.recv_sems.at[self.used],
            device_id=to,
            device_id_type=MESH,
        )
        self.used += 1
        copy.start()
        self.flying.append(copy)
        return copy

    def drain(self):
        for copy in self.flying:
            copy.wait_send()


def at(i, n):
    return pl.ds(pl.multiple_of(i * n, n), n)


def dot(a, b, dims=((1,), (0,))):
    return lax.dot_general(a, b, (dims, ((), ())), preferred_element_type=F32)


def pool_weights(plen, chip):
    lane = lax.broadcasted_iota(jnp.int32, (16, 16), 1)
    length = jnp.sum(jnp.where(lane == chip, plen[...], 0).astype(F32), axis=1, keepdims=True)
    slot = lax.broadcasted_iota(jnp.int32, (16, 1), 0).astype(F32)
    return jnp.where(slot < length, 1.0 / length, 0.0)


COPIES = sum(
    (2, 3, 6, 7, 3, 6, 1, 1, 15, 3, 12, 15, 7, 15, 15, 3, 12, 16, 1, 15, 15, 1, 15, 7, 8, 8, 1)
)
SCORE_SCALE = 256 ** (-0.5)
IMAGES = 512


def step_kernel(
    plen_h, tok_h, ngain_h, w_up_h, w_down_h, fgain_h, w_proj_h, quer_h, assign_h, valid_h,
    up_h, down_h, proj_h, qg_h,
    plen, tok, ngain, w_up, w_down, fgain, w_proj, quer, assign, valid,
    nrm, gd, cs, cr, xs, xr, ys, yr, lo, wfull, frow, psend, prow, allf, vcol, score, sgrad, qg, up_o, down_o, proj_o,
    fcs, fcr, ts, tr, ps, pr, fgb, gs, cols, scg, gz, pj, pjf, oh, og, h_all, n_t, ohz, dg, dp, dpr,
    us, uyr, uz, ur, load_sems, store_sems, send_sems, recv_sems,
):
    me = Place()
    send = Sends(send_sems, recv_sems)
    core, chip, x, y, t, z, yl = me.core, me.chip, me.x, me.y, me.t, me.z, me.yl
    loads = {}
    for n, (name, src, dst) in enumerate((
        ("tok", tok_h, tok), ("ngain", ngain_h, ngain), ("w_up", w_up_h, w_up), ("w_down", w_down_h, w_down),
        ("w_proj", w_proj_h, w_proj), ("plen", plen_h, plen), ("fgain", fgain_h, fgain),
        ("quer", quer_h, quer), ("assign", assign_h, assign), ("valid", valid_h, valid),
    )):
        loads[name] = pltpu.make_async_copy(src, dst, load_sems.at[n])
        loads[name].start()
    me.greet()
    stores = []

    def store(src, dst):
        copy = pltpu.make_async_copy(src, dst, store_sems.at[len(stores)])
        copy.start()
        stores.append(copy)

    loads["tok"].wait()
    loads["ngain"].wait()
    tokens = tok[...].astype(F32)
    centred = tokens - jnp.mean(tokens, axis=1, keepdims=True)
    variance = jnp.mean(centred * centred, axis=1, keepdims=True)
    normed = (centred * lax.rsqrt(variance + EPS) * ngain[...]).astype(BF16)
    nrm[...] = normed
    loads["w_up"].wait()
    pre = dot(normed, w_up[...])
    tanh = jnp.tanh(GC * (pre + GA * pre * pre * pre))
    hidden = (0.5 * pre * (1.0 + tanh)).astype(BF16)
    gd[...] = 0.5 * (1.0 + tanh) + 0.5 * pre * (1.0 - tanh * tanh) * (GC * (1.0 + 3.0 * GA * pre * pre))
    loads["w_proj"].wait()
    loads["w_down"].wait()
    wfull[y, x, core] = w_proj[...]
    for j in range(2):
        cs[j] = dot(hidden, w_down[:, at((1 - core) * 2 + j, 512)]).astype(BF16)
    h_all[z] = hidden.T
    me.met()
    to_core = [send(cs.at[j], cr.at[j], me.other_core()) for j in range(2)]
    w_y = [send(w_proj, wfull.at[y, x, core], me.along_y(i)) for i in (1, 2, 3)]
    to_x = []
    for j in range(2):
        own = dot(hidden, w_down[:, at(core * 2 + j, 512)])
        to_core[j].wait_recv()
        xs[j] = (own + cr[j].astype(F32)).astype(BF16).reshape(4, 4, 16, 512)
        to_x.append(
            [send(xs.at[j, :, lax.rem(x + i, 4)], xr.at[j, i - 1], me.along_x(i)) for i in (2, 1, 3)]
        )
    h_to = [send(h_all.at[z], h_all.at[z], me.along_z(i)) for i in (4, 3, 5, 2, 6, 1, 7)]
    for name in ("plen", "fgain", "quer", "assign", "valid"):
        loads[name].wait()
    vcol[...] = jnp.broadcast_to(valid[...].astype(F32), (128, 256)).T
    for copy in w_y:
        copy.wait_recv()
    w_x = [send(wfull.at[:, x, core], wfull.at[:, x, core], me.along_x(i)) for i in (1, 2, 3)]
    to_y = []
    for j in range(2):
        for copy in to_x[j]:
            copy.wait_recv()
        total = xs[j, :, x].astype(F32)
        for i in range(3):
            total += xr[j, i].astype(F32)
        ys[j] = total.astype(BF16)
        to_y.append([send(ys.at[j, lax.rem(y + i, 4)], yr.at[j, i - 1], me.along_y(i)) for i in (2, 1, 3)])
    for copy in w_x:
        copy.wait_recv()
    w_core = send(wfull.at[:, :, core], wfull.at[:, :, core], me.other_core())
    for j in range(2):
        for copy in to_y[j]:
            copy.wait_recv()
        total = ys[j, y].astype(F32)
        for i in range(3):
            total += yr[j, i].astype(F32)
        lo[core, :, j * 512 : (j + 1) * 512] = total
    half = send(lo.at[core], lo.at[core], me.other_core())
    half.wait_recv()
    layer_out = tok[at(chip, 16), :].astype(F32) + jnp.concatenate([lo[0], lo[1]], axis=1)
    centred = layer_out - jnp.mean(layer_out, axis=1, keepdims=True)
    inv_scale = lax.rsqrt(jnp.mean(centred * centred, axis=1, keepdims=True) + EPS)
    out_hat = centred * inv_scale
    final = out_hat * fgain[...]
    pool_weight = pool_weights(plen, chip)
    pooled = jnp.sum(final * pool_weight, axis=0, keepdims=True)
    pooled_low = pooled.astype(BF16)
    w_core.wait_recv()
    feat = dot(jnp.broadcast_to(pooled_low, (16, 2048)), wfull[...].reshape(2048, 256))
    frow[chip] = feat[:1].astype(BF16).astype(F32)
    to_plane = [send(frow.at[chip], frow.at[chip], me.in_plane(i)) for i in range(1, 16)]
    hat_low = out_hat.astype(BF16)
    oh[0, chip] = hat_low[:, :1024]
    oh[1, chip] = hat_low[:, 1024:]
    own = oh.at[core, chip]
    oh_y = [send(own, own, me.along_y(i)) for i in (2, 1, 3)]
    oh_waves = [[send(own, own, me.along_x(i)) for i in (2, 1, 3)]]
    for k in range(16):
        ohz[k] = hat_low[:, 128 * k : 128 * k + 128]
    dg[core, chip, z] = ohz[2 * z + core]
    z_to = [
        send(ohz.at[lax.rem(z + i, 8) * 2 + core], dg.at[core, chip, z], me.along_z(i))
        for i in (4, 3, 5, 2, 6, 1, 7)
    ]
    rounded = pooled_low.astype(F32)
    diagonal = lax.broadcasted_iota(jnp.int32, (16, 128), 0) == lax.broadcasted_iota(jnp.int32, (16, 128), 1)
    scale_row = jnp.sum(jnp.where(diagonal, pool_weight * inv_scale, 0.0), axis=0, keepdims=True)
    for k in range(16):
        psend[k] = jnp.concatenate([rounded[:, k * 128 : (k + 1) * 128], scale_row], axis=1)
    prow[chip] = psend[chip]
    pooled_to = [send(psend.at[lax.rem(chip + i, 16)], prow.at[chip], me.in_plane(i)) for i in range(1, 16)]
    n_t[...] = nrm[...].T
    for copy in to_plane:
        copy.wait_recv()
    allf[t] = jnp.concatenate([frow[k] for k in range(16)], axis=0).astype(BF16)
    to_text = [send(allf.at[t], allf.at[t], me.in_text(i)) for i in range(1, 16)]

    def spread_y(to_y, buf, waves, to_other):
        for copy, i in ((to_y[1], 1), (to_y[2], 3), (to_y[0], 2)):
            copy.wait_recv()
            block = buf.at[core, lax.rem(y + 4 - i, 4) * 4 + x]
            waves.append([send(block, block, me.along_x(j)) for j in (2, 1, 3)])
            to_other.append(send(block, block, me.other_core()))

    def spread_x(buf, waves, to_other):
        for wave, i in zip(waves, (0, 1, 3, 2)):
            for copy, j in zip(wave, (2, 1, 3)):
                copy.wait_recv()
                block = buf.at[core, lax.rem(y + 4 - i, 4) * 4 + lax.rem(x + 4 - j, 4)]
                to_other.append(send(block, block, me.other_core()))

    oh_other = []
    spread_y(oh_y, oh, oh_waves, oh_other)
    for copy in pooled_to:
        copy.wait_recv()
    pj[t, :, 256:] = jnp.concatenate([prow[k] for k in range(16)], axis=0)[:, :128].astype(BF16)
    for copy in z_to:
        copy.wait_recv()
    own = dg.at[core, chip]
    dg_y = [send(own, own, me.along_y(i)) for i in (2, 1, 3)]
    dg_waves = [[send(own, own, me.along_x(i)) for i in (2, 1, 3)]]
    dg_other = [send(own, own, me.other_core())]
    chosen = assign[...]

    def query_half(half, start):
        blocks = [lax.rem(t + start + n, 16) for n in range(8)]
        for n in range(8):
            back = (16 - start - n) % 16
            if back:
                to_text[back - 1].wait_recv()
        score[half] = dot(jnp.concatenate([allf[b] for b in blocks], axis=0), quer[...], ((1,), (1,)))

        @pl.loop(0, 8)
        def _(n):
            block = lax.rem(t + start + n, 16)
            spot = at(block, 16)
            s = score[half, at(n, 16), :] * SCORE_SCALE + LOGIT_BIAS
            concept = lax.broadcasted_iota(jnp.int32, (16, 1100), 0) + block * 16
            hit = concept == chosen
            u = jnp.where(hit, -s, s)
            e = jnp.exp(-jnp.abs(u))
            more = 1.0 / (1.0 + e)
            less = e * more
            p = jnp.where(u >= 0.0, more, less)
            q = jnp.where(u >= 0.0, less, more)
            soft = jnp.maximum(u, 0.0) + jnp.log1p(e)
            factor = jnp.where(hit, -ALPHA, 1.0 - ALPHA) * vcol[spot, :1]
            sgrad[spot, :] = (factor * p * p * (p + 2.0 * q * soft)).astype(BF16)

    query_half(0, 13)
    query_half(1, 5)
    terms = dot(sgrad[...], quer[...]) * (SCORE_SCALE / IMAGES)
    halves = (terms[:, :128], terms[:, 128:])
    mine = jnp.where(core == 0, halves[0], halves[1])
    fcs[...] = jnp.where(core == 0, halves[1], halves[0]).astype(BF16)
    to_core = send(fcs, fcr, me.other_core())
    spread_y(dg_y, dg, dg_waves, dg_other)
    to_core.wait_recv()
    ts[...] = (mine + fcr[...].astype(F32)).astype(BF16).reshape(16, 16, 128)
    to_text2 = [send(ts.at[lax.rem(t + i, 16)], tr.at[i - 1], me.in_text(i)) for i in range(1, 16)]
    query_grad = dot(sgrad[...], allf[...].reshape(256, 256), ((0,), (0,))) * SCORE_SCALE
    qg[pl.ds(0, 1100, stride=2), :] = query_grad[:, :128]
    qg[pl.ds(1, 1100, stride=2), :] = query_grad[:, 128:]
    store(qg, qg_h)
    spread_x(oh, oh_waves, oh_other)
    for copy in oh_other:
        copy.wait_recv()
    total = ts[t].astype(F32)
    for i in range(15):
        to_text2[i].wait_recv()
        total += tr[i].astype(F32)
    ps[...] = total.astype(BF16)
    to_plane2 = [send(ps, pr.at[i - 1], me.in_plane(i)) for i in range(1, 16)]
    spread_x(dg, dg_waves, dg_other)
    for i in range(15):
        to_plane2[i].wait_recv()
        total += pr[i].astype(F32)
    fgb[core] = total
    half = send(fgb.at[core], fgb.at[core], me.other_core())
    half.wait_recv()
    feat_grad = jnp.concatenate([fgb[0], fgb[1]], axis=1)
    pj[t, :, :256] = feat_grad.astype(BF16)
    pj_to = [send(pj.at[t], pj.at[t], me.in_text(i)) for i in range(1, 16)]
    high = feat_grad.astype(BF16)
    middle = (feat_grad - high.astype(F32)).astype(BF16)
    low = (feat_grad - high.astype(F32) - middle.astype(F32)).astype(BF16)
    parts = dot(jnp.concatenate([high, middle, low], axis=0), wfull[...].reshape(2048, 256), ((1,), (1,)))
    gs[...] = (parts[:16] + parts[16:32] + parts[32:]) * fgain[...]
    lane = lax.broadcasted_iota(jnp.int32, (16, 128), 1)
    for k in range(16):
        hat = gs[k : k + 1, :]
        out_hat = jnp.concatenate([oh[0, k], oh[1, k]], axis=1).astype(F32)
        first = jnp.mean(hat, axis=1, keepdims=True)
        second = jnp.mean(hat * out_hat, axis=1, keepdims=True)
        scale = jnp.sum(jnp.where(diagonal, prow[k][:, 128:], 0.0), axis=1, keepdims=True)
        og[16 * k : 16 * k + 16, :] = ((hat - first - out_hat * second) * scale).astype(BF16)
        cols[16 * k : 16 * k + 16, :] = jnp.where(
            lane == 0, scale, jnp.where(lane == 1, first, jnp.where(lane == 2, second, 0.0))
        )
    scg[z] = cols[...].T[:8]
    sc_to = [send(scg.at[z], scg.at[z], me.along_z(i)) for i in (4, 3, 5, 2, 6, 1, 7)]
    hidden_grad = dot(og[...], w_down[...], ((1,), (1,)))
    pre_grad = (hidden_grad * gd[...]).astype(BF16)
    us[...] = dot(n_t[...], pre_grad).astype(BF16).reshape(8, 2, 128, 256)
    order = (4, 3, 5, 2, 6, 1, 7, 0)
    up_y = {}
    for i in order:
        up_y[i] = send(us.at[lax.rem(z + i, 8), 1 - yl], uyr.at[i], me.across())

    def pair_sum(i):
        up_y[i].wait_recv()
        return us[lax.rem(z + i, 8), yl].astype(F32) + uyr[i].astype(F32)

    near, far = pl.ds(0, 64), pl.ds(64, 64)
    uz[3] = pair_sum(4).astype(BF16)
    relay = {
        2: send(uz.at[3, near], ur.at[4, near], me.along_z(2)),
        6: send(uz.at[3, far], ur.at[4, far], me.along_z(6)),
    }
    for i, via, to in ((3, 2, 1), (5, 6, 7)):
        uz[i - 1] = pair_sum(i).astype(BF16)
        relay[to] = send(uz.at[i - 1], ur.at[5 if i == 3 else 6], me.along_z(via))
    for copy in dg_other + h_to + sc_to + pj_to:
        copy.wait_recv()
    fg_group = jnp.concatenate([pj[2 * k + yl, :, :256] for k in range(8)], axis=0)
    w_group = wfull[z // 2, pl.ds(2 * lax.rem(z, 2), 2)].reshape(256, 256)
    gz[...] = dot(fg_group, w_group, ((1,), (1,))) * fgain[:, at(z, 256)]
    product = jnp.zeros((256, 256), F32)
    for k in range(8):
        turned = jnp.concatenate([scg[k], jnp.zeros((120, 256), F32)], axis=0).T
        scale, first, second = turned[:, :1], turned[:, 1:2], turned[:, 2:3]
        hat = jnp.broadcast_to(gz[16 * k : 16 * k + 16][:, None, :], (16, 16, 256)).reshape(256, 256)
        out_hat = jnp.concatenate([dg[h, :, k].reshape(256, 128) for h in range(2)], axis=1).astype(F32)
        grads = ((hat - first - out_hat * second) * scale).astype(BF16)
        product += dot(h_all[k], grads)
    lower, upper = product[:, :128], product[:, 128:]
    dp[...] = jnp.where(yl == 0, upper, lower).astype(BF16)
    down_own = jnp.where(yl == 0, lower, upper)
    dp_to = send(dp, dpr, me.across())
    last = {}
    for i in (2, 6, 1, 7):
        total = pair_sum(i)
        relay[i].wait_recv()
        if i == 2:
            uz[1, near] = (total[:64] + ur[4, near].astype(F32)).astype(BF16)
            uz[1, far] = total[64:].astype(BF16)
        elif i == 6:
            uz[5, near] = total[:64].astype(BF16)
            uz[5, far] = (total[64:] + ur[4, far].astype(F32)).astype(BF16)
        else:
            uz[i - 1] = (total + ur[5 if i == 1 else 6].astype(F32)).astype(BF16)
        last[i] = send(uz.at[i - 1], ur.at[(2, 6, 1, 7).index(i)], me.along_z(i))
    pjf[...] = dot(pj[:, :, 256:].reshape(256, 128), pj[:, :, :256].reshape(256, 256), ((0,), (0,)))
    proj_o[...] = pjf[at(core, 64), :]
    store(proj_o, proj_h)
    dp_to.wait_recv()
    down_o[...] = down_own + dpr[...].astype(F32)
    store(down_o, down_h)
    total = pair_sum(0)
    for n, i in enumerate((2, 6, 1, 7)):
        last[i].wait_recv()
        total += ur[n].astype(F32)
    up_o[...] = total
    store(up_o, up_h)
    send.drain()
    for copy in stores:
        copy.wait()


def hand_out_kernel(a, b, c, d, a_o, b_o, c_o, d_o, a_v, b_v, c_v, d_v, sems):
    parts = []
    for lo, n in ((0, 552), (552, 552), (1104, 552), (1656, 544)):
        rows = pl.ds(lo, n)
        parts.append((d.at[rows], d_v.at[rows], d_o.at[rows]))
    parts += [(a, a_v, a_o), (b, b_v, b_o), (c, c_v, c_o)]
    loads = [pltpu.make_async_copy(src, mid, sems.at[0, n]) for n, (src, mid, _) in enumerate(parts)]
    stores = [pltpu.make_async_copy(mid, dst, sems.at[1, n]) for n, (_, mid, dst) in enumerate(parts)]
    for load in loads:
        load.start()
    for load, store in zip(loads, stores):
        load.wait()
        store.start()
    for store in stores:
        store.wait()


def hand_out(arrays):
    return pl.pallas_call(
        hand_out_kernel,
        name="hand_out",
        in_specs=[pl.BlockSpec(memory_space=pltpu.HBM)] * 4,
        out_specs=[pl.BlockSpec(memory_space=pltpu.HBM)] * 4,
        out_shape=[jax.ShapeDtypeStruct(a.shape, a.dtype) for a in arrays],
        scratch_shapes=[pltpu.VMEM(a.shape, a.dtype) for a in arrays] + [pltpu.SemaphoreType.DMA((2, 7))],
        compiler_params=pltpu.CompilerParams(vmem_limit_bytes=62 << 20),
    )(*arrays)


def step(*args):
    return pl.pallas_call(
        step_kernel,
        name="step",
        in_specs=[pl.BlockSpec(memory_space=pltpu.HBM)] * 10,
        out_specs=[pl.BlockSpec(memory_space=pltpu.HBM)] * 4,
        out_shape=(
            jax.ShapeDtypeStruct((128, 256), F32),
            jax.ShapeDtypeStruct((256, 128), F32),
            jax.ShapeDtypeStruct((64, 256), F32),
            jax.ShapeDtypeStruct((2200, 128), F32),
        ),
        scratch_shapes=[
            pltpu.VMEM((1, 16), jnp.int32),
            pltpu.VMEM((256, 2048), BF16),
            pltpu.VMEM((1, 2048), F32),
            pltpu.VMEM((2048, 256), BF16),
            pltpu.VMEM((256, 2048), BF16),
            pltpu.VMEM((1, 2048), F32),
            pltpu.VMEM((64, 256), BF16),
            pltpu.VMEM((1100, 256), BF16),
            pltpu.VMEM((1, 1100), jnp.int32),
            pltpu.VMEM((1, 256), jnp.int32),
            pltpu.VMEM((256, 2048), BF16),
            pltpu.VMEM((256, 256), F32),
            pltpu.VMEM((2, 256, 512), BF16),
            pltpu.VMEM((2, 256, 512), BF16),
            pltpu.VMEM((2, 4, 4, 16, 512), BF16),
            pltpu.VMEM((2, 3, 4, 16, 512), BF16),
            pltpu.VMEM((2, 4, 16, 512), BF16),
            pltpu.VMEM((2, 3, 16, 512), BF16),
            pltpu.VMEM((2, 16, 1024), F32),
            pltpu.VMEM((4, 4, 2, 64, 256), BF16),
            pltpu.VMEM((16, 1, 256), F32),
            pltpu.VMEM((16, 1, 256), F32),
            pltpu.VMEM((16, 1, 256), F32),
            pltpu.VMEM((16, 16, 256), BF16),
            pltpu.VMEM((256, 128), F32),
            pltpu.VMEM((2, 128, 1100), F32),
            pltpu.VMEM((256, 1100), BF16),
            pltpu.VMEM((2200, 128), F32),
            pltpu.VMEM((128, 256), F32),
            pltpu.VMEM((256, 128), F32),
            pltpu.VMEM((64, 256), F32),
            pltpu.VMEM((256, 128), BF16),
            pltpu.VMEM((256, 128), BF16),
            pltpu.VMEM((16, 16, 128), BF16),
            pltpu.VMEM((15, 16, 128), BF16),
            pltpu.VMEM((16, 128), BF16),
            pltpu.VMEM((15, 16, 128), BF16),
            pltpu.VMEM((2, 16, 128), F32),
            pltpu.VMEM((16, 2048), F32),
            pltpu.VMEM((256, 128), F32),
            pltpu.VMEM((8, 8, 256), F32),
            pltpu.VMEM((128, 256), F32),
            pltpu.VMEM((16, 16, 384), BF16),
            pltpu.VMEM((128, 256), F32),
            pltpu.VMEM((2, 16, 16, 1024), BF16),
            pltpu.VMEM((256, 2048), BF16),
            pltpu.VMEM((8, 256, 256), BF16),
            pltpu.VMEM((2048, 256), BF16),
            pltpu.VMEM((16, 16, 128), BF16),
            pltpu.VMEM((2, 16, 8, 16, 128), BF16),
            pltpu.VMEM((256, 128), BF16),
            pltpu.VMEM((256, 128), BF16),
            pltpu.VMEM((8, 2, 128, 256), BF16),
            pltpu.VMEM((8, 128, 256), BF16),
            pltpu.VMEM((7, 128, 256), BF16),
            pltpu.VMEM((7, 128, 256), BF16),
            pltpu.SemaphoreType.DMA((10,)),
            pltpu.SemaphoreType.DMA((4,)),
            pltpu.SemaphoreType.DMA((COPIES,)),
            pltpu.SemaphoreType.DMA((COPIES,)),
        ],
        compiler_params=pltpu.CompilerParams(
            collective_id=0, has_side_effects=True, vmem_limit_bytes=62 << 20
        ),
    )(*args)


def body(
    prompt_embeds, prompt_len, norm_gain, w_up, w_down, final_gain, w_proj, queries, assign, valid
):
    results = step(
        prompt_len.reshape(1, 16),
        prompt_embeds.reshape(256, 2048),
        norm_gain.reshape(1, 2048),
        w_up,
        w_down,
        final_gain.reshape(1, 2048),
        w_proj,
        queries.reshape(1100, 256),
        assign,
        valid,
    )
    up_grad, down_grad, proj_grad, query_grad = hand_out(results)
    return (up_grad, down_grad, proj_grad, query_grad.reshape(1, 1100, 256))


def solution(mesh):
    return jax.shard_map(
        body,
        mesh=mesh,
        in_specs=(
            P("text", None, None),
            P("text"),
            P(),
            P(None, "det"),
            P("det", None),
            P(),
            P("det", None),
            P(("text", "det"), None, None),
            P(("text", "det"), None),
            P(("text", "det"), None),
        ),
        out_specs=(
            P("text", "det"),
            P("det", "text"),
            P("det", None),
            P(("text", "det"), None, None),
        ),
        check_vma=False,
    )
```

```python
import jax
import jax.numpy as jnp
from jax import lax
from jax.experimental import pallas as pl
from jax.experimental.pallas import tpu as pltpu
from jax.sharding import PartitionSpec as P

EPS = 1e-05
ALPHA = 0.25
LOGIT_BIAS = -2.0
F32 = jnp.float32
BF16 = jnp.bfloat16
MESH = pl.DeviceIdType.MESH
GC = 0.7978845608028654
GA = 0.044715


class Place:
    def __init__(self):
        self.t = lax.axis_index("text")
        self.d = lax.axis_index("det")
        self.core = lax.rem(self.d, 2)
        self.chip = self.d // 2
        self.x = lax.rem(self.chip, 4)
        self.y = self.chip // 4
        self.z = self.t // 2
        self.yl = lax.rem(self.t, 2)

    def other_core(self):
        return {"det": self.d + 1 - 2 * self.core}

    def along_x(self, i):
        return {"det": (self.y * 4 + lax.rem(self.x + i, 4)) * 2 + self.core}

    def along_y(self, i):
        return {"det": (lax.rem(self.y + i, 4) * 4 + self.x) * 2 + self.core}

    def in_plane(self, i):
        return {"det": lax.rem(self.chip + i, 16) * 2 + self.core}

    def in_text(self, i):
        return {"text": lax.rem(self.t + i, 16)}

    def along_z(self, i):
        return {"text": lax.rem(self.z + i, 8) * 2 + self.yl}

    def across(self):
        return {"text": self.t + 1 - 2 * self.yl}

    def greet(self):
        barrier = pltpu.get_barrier_semaphore()
        pl.semaphore_signal(barrier, inc=1, device_id=self.other_core(), device_id_type=MESH)
        for i in range(1, 16):
            pl.semaphore_signal(barrier, inc=1, device_id=self.in_plane(i), device_id_type=MESH)
            pl.semaphore_signal(barrier, inc=1, device_id=self.in_text(i), device_id_type=MESH)

    def met(self):
        pl.semaphore_wait(pltpu.get_barrier_semaphore(), 31)


class Sends:
    def __init__(self, send_sems, recv_sems):
        self.send_sems, self.recv_sems, self.used = send_sems, recv_sems, 0
        self.flying = []

    def __call__(self, src, dst, to):
        copy = pltpu.make_async_remote_copy(
            src_ref=src,
            dst_ref=dst,
            send_sem=self.send_sems.at[self.used],
            recv_sem=self.recv_sems.at[self.used],
            device_id=to,
            device_id_type=MESH,
        )
        self.used += 1
        copy.start()
        self.flying.append(copy)
        return copy

    def drain(self):
        for copy in self.flying:
            copy.wait_send()


def at(i, n):
    return pl.ds(pl.multiple_of(i * n, n), n)


def dot(a, b, dims=((1,), (0,))):
    return lax.dot_general(a, b, (dims, ((), ())), preferred_element_type=F32)


def pool_weights(plen, chip):
    lane = lax.broadcasted_iota(jnp.int32, (16, 16), 1)
    length = jnp.sum(jnp.where(lane == chip, plen[...], 0).astype(F32), axis=1, keepdims=True)
    slot = lax.broadcasted_iota(jnp.int32, (16, 1), 0).astype(F32)
    return jnp.where(slot < length, 1.0 / length, 0.0)


COPIES = sum(
    (2, 3, 6, 7, 3, 6, 1, 1, 15, 3, 12, 15, 7, 15, 15, 3, 12, 16, 1, 15, 15, 1, 15, 7, 8, 8, 1)
)
SCORE_SCALE = 256 ** (-0.5)
IMAGES = 512


def step_kernel(
    plen_h, tok_h, ngain_h, w_up_h, w_down_h, fgain_h, w_proj_h, quer_h, assign_h, valid_h,
    up_h, down_h, proj_h, qg_h,
    plen, tok, ngain, w_up, w_down, fgain, w_proj, quer, assign, valid,
    nrm, gd, cs, cr, xs, xr, ys, yr, lo, wfull, frow, psend, prow, allf, vcol, score, sgrad, qg, up_o, down_o, proj_o,
    fcs, fcr, ts, tr, ps, pr, fgb, gs, cols, scg, gz, pj, pjf, oh, og, h_all, n_t, ohz, dg, dp, dpr,
    us, uyr, uz, ur, load_sems, store_sems, send_sems, recv_sems,
):
    me = Place()
    send = Sends(send_sems, recv_sems)
    core, chip, x, y, t, z, yl = me.core, me.chip, me.x, me.y, me.t, me.z, me.yl
    loads = {}
    for n, (name, src, dst) in enumerate((
        ("tok", tok_h, tok), ("ngain", ngain_h, ngain), ("w_up", w_up_h, w_up), ("w_down", w_down_h, w_down),
        ("w_proj", w_proj_h, w_proj), ("plen", plen_h, plen), ("fgain", fgain_h, fgain),
        ("quer", quer_h, quer), ("assign", assign_h, assign), ("valid", valid_h, valid),
    )):
        loads[name] = pltpu.make_async_copy(src, dst, load_sems.at[n])
        loads[name].start()
    me.greet()
    stores = []

    def store(src, dst):
        copy = pltpu.make_async_copy(src, dst, store_sems.at[len(stores)])
        copy.start()
        stores.append(copy)

    loads["tok"].wait()
    loads["ngain"].wait()
    tokens = tok[...].astype(F32)
    centred = tokens - jnp.mean(tokens, axis=1, keepdims=True)
    variance = jnp.mean(centred * centred, axis=1, keepdims=True)
    normed = (centred * lax.rsqrt(variance + EPS) * ngain[...]).astype(BF16)
    nrm[...] = normed
    loads["w_up"].wait()
    pre = dot(normed, w_up[...])
    tanh = jnp.tanh(GC * (pre + GA * pre * pre * pre))
    hidden = (0.5 * pre * (1.0 + tanh)).astype(BF16)
    gd[...] = 0.5 * (1.0 + tanh) + 0.5 * pre * (1.0 - tanh * tanh) * (GC * (1.0 + 3.0 * GA * pre * pre))
    loads["w_proj"].wait()
    loads["w_down"].wait()
    wfull[y, x, core] = w_proj[...]
    for j in range(2):
        cs[j] = dot(hidden, w_down[:, at((1 - core) * 2 + j, 512)]).astype(BF16)
    h_all[z] = hidden.T
    me.met()
    to_core = [send(cs.at[j], cr.at[j], me.other_core()) for j in range(2)]
    w_y = [send(w_proj, wfull.at[y, x, core], me.along_y(i)) for i in (1, 2, 3)]
    to_x = []
    for j in range(2):
        own = dot(hidden, w_down[:, at(core * 2 + j, 512)])
        to_core[j].wait_recv()
        xs[j] = (own + cr[j].astype(F32)).astype(BF16).reshape(4, 4, 16, 512)
        to_x.append(
            [send(xs.at[j, :, lax.rem(x + i, 4)], xr.at[j, i - 1], me.along_x(i)) for i in (2, 1, 3)]
        )
    h_to = [send(h_all.at[z], h_all.at[z], me.along_z(i)) for i in (4, 3, 5)]
    for name in ("plen", "fgain", "quer", "assign", "valid"):
        loads[name].wait()
    vcol[...] = jnp.broadcast_to(valid[...].astype(F32), (128, 256)).T
    for copy in w_y:
        copy.wait_recv()
    w_x = [send(wfull.at[:, x, core], wfull.at[:, x, core], me.along_x(i)) for i in (1, 2, 3)]
    to_y = []
    for j in range(2):
        for copy in to_x[j]:
            copy.wait_recv()
        total = xs[j, :, x].astype(F32)
        for i in range(3):
            total += xr[j, i].astype(F32)
        ys[j] = total.astype(BF16)
        to_y.append([send(ys.at[j, lax.rem(y + i, 4)], yr.at[j, i - 1], me.along_y(i)) for i in (2, 1, 3)])
    for copy in w_x:
        copy.wait_recv()
    w_core = send(wfull.at[:, :, core], wfull.at[:, :, core], me.other_core())
    for j in range(2):
        for copy in to_y[j]:
            copy.wait_recv()
        total = ys[j, y].astype(F32)
        for i in range(3):
            total += yr[j, i].astype(F32)
        lo[core, :, j * 512 : (j + 1) * 512] = total
    half = send(lo.at[core], lo.at[core], me.other_core())
    half.wait_recv()
    layer_out = tok[at(chip, 16), :].astype(F32) + jnp.concatenate([lo[0], lo[1]], axis=1)
    centred = layer_out - jnp.mean(layer_out, axis=1, keepdims=True)
    inv_scale = lax.rsqrt(jnp.mean(centred * centred, axis=1, keepdims=True) + EPS)
    out_hat = centred * inv_scale
    final = out_hat * fgain[...]
    pool_weight = pool_weights(plen, chip)
    pooled = jnp.sum(final * pool_weight, axis=0, keepdims=True)
    pooled_low = pooled.astype(BF16)
    w_core.wait_recv()
    feat = dot(jnp.broadcast_to(pooled_low, (16, 2048)), wfull[...].reshape(2048, 256))
    frow[chip] = feat[:1].astype(BF16).astype(F32)
    to_plane = [send(frow.at[chip], frow.at[chip], me.in_plane(i)) for i in range(1, 16)]
    hat_low = out_hat.astype(BF16)
    oh[0, chip] = hat_low[:, :1024]
    oh[1, chip] = hat_low[:, 1024:]
    own = oh.at[core, chip]
    oh_y = [send(own, own, me.along_y(i)) for i in (2, 1, 3)]
    oh_waves = [[send(own, own, me.along_x(i)) for i in (2, 1, 3)]]
    for k in range(16):
        ohz[k] = hat_low[:, 128 * k : 128 * k + 128]
    dg[core, chip, z] = ohz[2 * z + core]
    z_to = [
        send(ohz.at[lax.rem(z + i, 8) * 2 + core], dg.at[core, chip, z], me.along_z(i))
        for i in (4, 3, 5, 2, 6, 1, 7)
    ]
    rounded = pooled_low.astype(F32)
    diagonal = lax.broadcasted_iota(jnp.int32, (16, 128), 0) == lax.broadcasted_iota(jnp.int32, (16, 128), 1)
    scale_row = jnp.sum(jnp.where(diagonal, pool_weight * inv_scale, 0.0), axis=0, keepdims=True)
    for k in range(16):
        psend[k] = jnp.concatenate([rounded[:, k * 128 : (k + 1) * 128], scale_row], axis=1)
    prow[chip] = psend[chip]
    pooled_to = [send(psend.at[lax.rem(chip + i, 16)], prow.at[chip], me.in_plane(i)) for i in range(1, 16)]
    n_t[...] = nrm[...].T
    for copy in to_plane:
        copy.wait_recv()
    allf[t] = jnp.concatenate([frow[k] for k in range(16)], axis=0).astype(BF16)
    to_text = [send(allf.at[t], allf.at[t], me.in_text(i)) for i in range(1, 16)]

    def spread_y(to_y, buf, waves, to_other):
        for copy, i in ((to_y[1], 1), (to_y[2], 3), (to_y[0], 2)):
            copy.wait_recv()
            block = buf.at[core, lax.rem(y + 4 - i, 4) * 4 + x]
            waves.append([send(block, block, me.along_x(j)) for j in (2, 1, 3)])
            to_other.append(send(block, block, me.other_core()))

    def spread_x(buf, waves, to_other):
        for wave, i in zip(waves, (0, 1, 3, 2)):
            for copy, j in zip(wave, (2, 1, 3)):
                copy.wait_recv()
                block = buf.at[core, lax.rem(y + 4 - i, 4) * 4 + lax.rem(x + 4 - j, 4)]
                to_other.append(send(block, block, me.other_core()))

    oh_other = []
    spread_y(oh_y, oh, oh_waves, oh_other)
    chosen = assign[...]

    def query_half(half, start):
        blocks = [lax.rem(t + start + n, 16) for n in range(8)]
        for n in range(8):
            back = (16 - start - n) % 16
            if back:
                to_text[back - 1].wait_recv()
        score[half] = dot(jnp.concatenate([allf[b] for b in blocks], axis=0), quer[...], ((1,), (1,)))

        @pl.loop(0, 8)
        def _(n):
            block = lax.rem(t + start + n, 16)
            spot = at(block, 16)
            s = score[half, at(n, 16), :] * SCORE_SCALE + LOGIT_BIAS
            concept = lax.broadcasted_iota(jnp.int32, (16, 1100), 0) + block * 16
            hit = concept == chosen
            u = jnp.where(hit, -s, s)
            e = jnp.exp(-jnp.abs(u))
            more = 1.0 / (1.0 + e)
            less = e * more
            p = jnp.where(u >= 0.0, more, less)
            q = jnp.where(u >= 0.0, less, more)
            soft = jnp.maximum(u, 0.0) + jnp.log1p(e)
            factor = jnp.where(hit, -ALPHA, 1.0 - ALPHA) * vcol[spot, :1]
            sgrad[spot, :] = (factor * p * p * (p + 2.0 * q * soft)).astype(BF16)

    query_half(0, 13)
    query_half(1, 5)
    terms = dot(sgrad[...], quer[...]) * (SCORE_SCALE / IMAGES)
    halves = (terms[:, :128], terms[:, 128:])
    mine = jnp.where(core == 0, halves[0], halves[1])
    fcs[...] = jnp.where(core == 0, halves[1], halves[0]).astype(BF16)
    to_core = send(fcs, fcr, me.other_core())
    to_core.wait_recv()
    ts[...] = (mine + fcr[...].astype(F32)).astype(BF16).reshape(16, 16, 128)
    to_text2 = [send(ts.at[lax.rem(t + i, 16)], tr.at[i - 1], me.in_text(i)) for i in range(1, 16)]
    h_to += [send(h_all.at[z], h_all.at[z], me.along_z(i)) for i in (2, 6, 1, 7)]
    for copy in pooled_to:
        copy.wait_recv()
    pj[t, :, 256:] = jnp.concatenate([prow[k] for k in range(16)], axis=0)[:, :128].astype(BF16)
    for copy in z_to:
        copy.wait_recv()
    own = dg.at[core, chip]
    dg_y = [send(own, own, me.along_y(i)) for i in (2, 1, 3)]
    dg_waves = [[send(own, own, me.along_x(i)) for i in (2, 1, 3)]]
    dg_other = [send(own, own, me.other_core())]
    query_grad = dot(sgrad[...], allf[...].reshape(256, 256), ((0,), (0,))) * SCORE_SCALE
    qg[pl.ds(0, 1100, stride=2), :] = query_grad[:, :128]
    qg[pl.ds(1, 1100, stride=2), :] = query_grad[:, 128:]
    store(qg, qg_h)
    spread_x(oh, oh_waves, oh_other)
    for copy in oh_other:
        copy.wait_recv()
    total = ts[t].astype(F32)
    for i in range(15):
        to_text2[i].wait_recv()
        total += tr[i].astype(F32)
    ps[...] = total.astype(BF16)
    to_plane2 = [send(ps, pr.at[i - 1], me.in_plane(i)) for i in range(1, 16)]
    spread_y(dg_y, dg, dg_waves, dg_other)
    for i in range(15):
        to_plane2[i].wait_recv()
        total += pr[i].astype(F32)
    fgb[core] = total
    half = send(fgb.at[core], fgb.at[core], me.other_core())
    half.wait_recv()
    feat_grad = jnp.concatenate([fgb[0], fgb[1]], axis=1)
    pj[t, :, :256] = feat_grad.astype(BF16)
    pj_to = [send(pj.at[t], pj.at[t], me.in_text(i)) for i in range(1, 16)]
    high = feat_grad.astype(BF16)
    middle = (feat_grad - high.astype(F32)).astype(BF16)
    low = (feat_grad - high.astype(F32) - middle.astype(F32)).astype(BF16)
    parts = dot(jnp.concatenate([high, middle, low], axis=0), wfull[...].reshape(2048, 256), ((1,), (1,)))
    gs[...] = (parts[:16] + parts[16:32] + parts[32:]) * fgain[...]
    lane = lax.broadcasted_iota(jnp.int32, (16, 128), 1)
    for k in range(16):
        hat = gs[k : k + 1, :]
        out_hat = jnp.concatenate([oh[0, k], oh[1, k]], axis=1).astype(F32)
        first = jnp.mean(hat, axis=1, keepdims=True)
        second = jnp.mean(hat * out_hat, axis=1, keepdims=True)
        scale = jnp.sum(jnp.where(diagonal, prow[k][:, 128:], 0.0), axis=1, keepdims=True)
        og[16 * k : 16 * k + 16, :] = ((hat - first - out_hat * second) * scale).astype(BF16)
        cols[16 * k : 16 * k + 16, :] = jnp.where(
            lane == 0, scale, jnp.where(lane == 1, first, jnp.where(lane == 2, second, 0.0))
        )
    scg[z] = cols[...].T[:8]
    sc_to = [send(scg.at[z], scg.at[z], me.along_z(i)) for i in (4, 3, 5, 2, 6, 1, 7)]
    hidden_grad = dot(og[...], w_down[...], ((1,), (1,)))
    pre_grad = (hidden_grad * gd[...]).astype(BF16)
    us[...] = dot(n_t[...], pre_grad).astype(BF16).reshape(8, 2, 128, 256)
    order = (4, 3, 5, 2, 6, 1, 7, 0)
    up_y = {}
    for i in order:
        up_y[i] = send(us.at[lax.rem(z + i, 8), 1 - yl], uyr.at[i], me.across())

    spread_x(dg, dg_waves, dg_other)

    def pair_sum(i):
        up_y[i].wait_recv()
        return us[lax.rem(z + i, 8), yl].astype(F32) + uyr[i].astype(F32)

    near, far = pl.ds(0, 64), pl.ds(64, 64)
    uz[3] = pair_sum(4).astype(BF16)
    relay = {
        2: send(uz.at[3, near], ur.at[4, near], me.along_z(2)),
        6: send(uz.at[3, far], ur.at[4, far], me.along_z(6)),
    }
    for i, via, to in ((3, 2, 1), (5, 6, 7)):
        uz[i - 1] = pair_sum(i).astype(BF16)
        relay[to] = send(uz.at[i - 1], ur.at[5 if i == 3 else 6], me.along_z(via))
    for copy in dg_other + h_to + sc_to + pj_to:
        copy.wait_recv()
    fg_group = jnp.concatenate([pj[2 * k + yl, :, :256] for k in range(8)], axis=0)
    w_group = wfull[z // 2, pl.ds(2 * lax.rem(z, 2), 2)].reshape(256, 256)
    gz[...] = dot(fg_group, w_group, ((1,), (1,))) * fgain[:, at(z, 256)]
    product = jnp.zeros((256, 256), F32)
    for k in range(8):
        turned = jnp.concatenate([scg[k], jnp.zeros((120, 256), F32)], axis=0).T
        scale, first, second = turned[:, :1], turned[:, 1:2], turned[:, 2:3]
        hat = jnp.broadcast_to(gz[16 * k : 16 * k + 16][:, None, :], (16, 16, 256)).reshape(256, 256)
        out_hat = jnp.concatenate([dg[h, :, k].reshape(256, 128) for h in range(2)], axis=1).astype(F32)
        grads = ((hat - first - out_hat * second) * scale).astype(BF16)
        product += dot(h_all[k], grads)
    lower, upper = product[:, :128], product[:, 128:]
    dp[...] = jnp.where(yl == 0, upper, lower).astype(BF16)
    down_own = jnp.where(yl == 0, lower, upper)
    dp_to = send(dp, dpr, me.across())
    last = {}
    for i in (2, 6, 1, 7):
        total = pair_sum(i)
        relay[i].wait_recv()
        if i == 2:
            uz[1, near] = (total[:64] + ur[4, near].astype(F32)).astype(BF16)
            uz[1, far] = total[64:].astype(BF16)
        elif i == 6:
            uz[5, near] = total[:64].astype(BF16)
            uz[5, far] = (total[64:] + ur[4, far].astype(F32)).astype(BF16)
        else:
            uz[i - 1] = (total + ur[5 if i == 1 else 6].astype(F32)).astype(BF16)
        last[i] = send(uz.at[i - 1], ur.at[(2, 6, 1, 7).index(i)], me.along_z(i))
    pjf[...] = dot(pj[:, :, 256:].reshape(256, 128), pj[:, :, :256].reshape(256, 256), ((0,), (0,)))
    proj_o[...] = pjf[at(core, 64), :]
    store(proj_o, proj_h)
    dp_to.wait_recv()
    down_o[...] = down_own + dpr[...].astype(F32)
    store(down_o, down_h)
    total = pair_sum(0)
    for n, i in enumerate((2, 6, 1, 7)):
        last[i].wait_recv()
        total += ur[n].astype(F32)
    up_o[...] = total
    store(up_o, up_h)
    send.drain()
    for copy in stores:
        copy.wait()


def hand_out_kernel(a, b, c, d, a_o, b_o, c_o, d_o, a_v, b_v, c_v, d_v, sems):
    parts = []
    for lo, n in ((0, 552), (552, 552), (1104, 552), (1656, 544)):
        rows = pl.ds(lo, n)
        parts.append((d.at[rows], d_v.at[rows], d_o.at[rows]))
    parts += [(a, a_v, a_o), (b, b_v, b_o), (c, c_v, c_o)]
    loads = [pltpu.make_async_copy(src, mid, sems.at[0, n]) for n, (src, mid, _) in enumerate(parts)]
    stores = [pltpu.make_async_copy(mid, dst, sems.at[1, n]) for n, (_, mid, dst) in enumerate(parts)]
    for load in loads:
        load.start()
    for load, store in zip(loads, stores):
        load.wait()
        store.start()
    for store in stores:
        store.wait()


def hand_out(arrays):
    return pl.pallas_call(
        hand_out_kernel,
        name="hand_out",
        in_specs=[pl.BlockSpec(memory_space=pltpu.HBM)] * 4,
        out_specs=[pl.BlockSpec(memory_space=pltpu.HBM)] * 4,
        out_shape=[jax.ShapeDtypeStruct(a.shape, a.dtype) for a in arrays],
        scratch_shapes=[pltpu.VMEM(a.shape, a.dtype) for a in arrays] + [pltpu.SemaphoreType.DMA((2, 7))],
        compiler_params=pltpu.CompilerParams(vmem_limit_bytes=62 << 20),
    )(*arrays)


def step(*args):
    return pl.pallas_call(
        step_kernel,
        name="step",
        in_specs=[pl.BlockSpec(memory_space=pltpu.HBM)] * 10,
        out_specs=[pl.BlockSpec(memory_space=pltpu.HBM)] * 4,
        out_shape=(
            jax.ShapeDtypeStruct((128, 256), F32),
            jax.ShapeDtypeStruct((256, 128), F32),
            jax.ShapeDtypeStruct((64, 256), F32),
            jax.ShapeDtypeStruct((2200, 128), F32),
        ),
        scratch_shapes=[
            pltpu.VMEM((1, 16), jnp.int32),
            pltpu.VMEM((256, 2048), BF16),
            pltpu.VMEM((1, 2048), F32),
            pltpu.VMEM((2048, 256), BF16),
            pltpu.VMEM((256, 2048), BF16),
            pltpu.VMEM((1, 2048), F32),
            pltpu.VMEM((64, 256), BF16),
            pltpu.VMEM((1100, 256), BF16),
            pltpu.VMEM((1, 1100), jnp.int32),
            pltpu.VMEM((1, 256), jnp.int32),
            pltpu.VMEM((256, 2048), BF16),
            pltpu.VMEM((256, 256), F32),
            pltpu.VMEM((2, 256, 512), BF16),
            pltpu.VMEM((2, 256, 512), BF16),
            pltpu.VMEM((2, 4, 4, 16, 512), BF16),
            pltpu.VMEM((2, 3, 4, 16, 512), BF16),
            pltpu.VMEM((2, 4, 16, 512), BF16),
            pltpu.VMEM((2, 3, 16, 512), BF16),
            pltpu.VMEM((2, 16, 1024), F32),
            pltpu.VMEM((4, 4, 2, 64, 256), BF16),
            pltpu.VMEM((16, 1, 256), F32),
            pltpu.VMEM((16, 1, 256), F32),
            pltpu.VMEM((16, 1, 256), F32),
            pltpu.VMEM((16, 16, 256), BF16),
            pltpu.VMEM((256, 128), F32),
            pltpu.VMEM((2, 128, 1100), F32),
            pltpu.VMEM((256, 1100), BF16),
            pltpu.VMEM((2200, 128), F32),
            pltpu.VMEM((128, 256), F32),
            pltpu.VMEM((256, 128), F32),
            pltpu.VMEM((64, 256), F32),
            pltpu.VMEM((256, 128), BF16),
            pltpu.VMEM((256, 128), BF16),
            pltpu.VMEM((16, 16, 128), BF16),
            pltpu.VMEM((15, 16, 128), BF16),
            pltpu.VMEM((16, 128), BF16),
            pltpu.VMEM((15, 16, 128), BF16),
            pltpu.VMEM((2, 16, 128), F32),
            pltpu.VMEM((16, 2048), F32),
            pltpu.VMEM((256, 128), F32),
            pltpu.VMEM((8, 8, 256), F32),
            pltpu.VMEM((128, 256), F32),
            pltpu.VMEM((16, 16, 384), BF16),
            pltpu.VMEM((128, 256), F32),
            pltpu.VMEM((2, 16, 16, 1024), BF16),
            pltpu.VMEM((256, 2048), BF16),
            pltpu.VMEM((8, 256, 256), BF16),
            pltpu.VMEM((2048, 256), BF16),
            pltpu.VMEM((16, 16, 128), BF16),
            pltpu.VMEM((2, 16, 8, 16, 128), BF16),
            pltpu.VMEM((256, 128), BF16),
            pltpu.VMEM((256, 128), BF16),
            pltpu.VMEM((8, 2, 128, 256), BF16),
            pltpu.VMEM((8, 128, 256), BF16),
            pltpu.VMEM((7, 128, 256), BF16),
            pltpu.VMEM((7, 128, 256), BF16),
            pltpu.SemaphoreType.DMA((10,)),
            pltpu.SemaphoreType.DMA((4,)),
            pltpu.SemaphoreType.DMA((COPIES,)),
            pltpu.SemaphoreType.DMA((COPIES,)),
        ],
        compiler_params=pltpu.CompilerParams(
            collective_id=0, has_side_effects=True, vmem_limit_bytes=62 << 20
        ),
    )(*args)


def body(
    prompt_embeds, prompt_len, norm_gain, w_up, w_down, final_gain, w_proj, queries, assign, valid
):
    results = step(
        prompt_len.reshape(1, 16),
        prompt_embeds.reshape(256, 2048),
        norm_gain.reshape(1, 2048),
        w_up,
        w_down,
        final_gain.reshape(1, 2048),
        w_proj,
        queries.reshape(1100, 256),
        assign,
        valid,
    )
    up_grad, down_grad, proj_grad, query_grad = hand_out(results)
    return (up_grad, down_grad, proj_grad, query_grad.reshape(1, 1100, 256))


def solution(mesh):
    return jax.shard_map(
        body,
        mesh=mesh,
        in_specs=(
            P("text", None, None),
            P("text"),
            P(),
            P(None, "det"),
            P("det", None),
            P(),
            P("det", None),
            P(("text", "det"), None, None),
            P(("text", "det"), None),
            P(("text", "det"), None),
        ),
        out_specs=(
            P("text", "det"),
            P("det", "text"),
            P("det", None),
            P(("text", "det"), None, None),
        ),
        check_vma=False,
    )
```
